32 devices in a mesh: grp: 8 (over z, x), ep: 4 (over y, core).
Axes of the slice: x: 2, y: 2, z: 4, core: 2. Of those that a mesh axis runs over, the one named last changes fastest.
Arguments:
- out_grad: bfloat16 [256, 4096], P('grp', 'ep'), may hold values from -6 to 6
- expert_ids: int32 [256, 8], P('grp'), may hold values from 0 to 15, as said below
- router_logits: float32 [256, 16], P('grp'), may hold values from -5 to 5
- router_weight: bfloat16 [16, 4096], P(None, 'ep'), may hold values from -0.09375 to 0.09375
- expert_weight: bfloat16 [16, 4096, 1024], P('grp', 'ep'), may hold values from -0.1875 to 0.1875
- hidden_saved: bfloat16 [8, 512, 1024], P('grp'), may hold values from -6 to 6
Outputs:
- weight_grad: bfloat16 [16, 4096, 1024], P('grp', 'ep')
- hidden_grad: bfloat16 [8, 512, 1024], P('grp', 'ep')
- input_grad: bfloat16 [256, 4096], P('grp', 'ep')
The draws below stay inside these ranges and needn't reach their ends.
Inputs may be any that keep to these rules, and one draw needn't show every extreme that they name: `expert_ids`: each row names 8 different experts, lying in at most 4 of the 4 groups of 4 consecutive experts. In each aligned block of 32 rows no expert is named by more than 32 rows, and some expert is named by exactly 32.
All inputs are finite; a program needn't handle non-finite values.
Results may differ from the reference program's by a relative error of at most 0.02.
Values may be sent and summed in bfloat16 or wider, within the bound.
No kernel may reach another device: no remote copies, remote signals or barrier semaphores. Data moves between devices by JAX's collectives and lax.ppermute only.
A program may use at most 64 MiB of HBM per device.

```python
import jax
import jax.numpy as jnp
from jax import lax

D = 4096
FF = 1024
EXP_GRP = 2
TOPG = 4
TOPK = 8
EXPERTS = 16
GROUPS = 4
GROUP_EXP = 4
PICK = 2
ROWS_GRP = 32
TOKENS = 256
USERS = 32
CAP = 32
SLOTS = 512
N_GRP = 8
N_EP = 4


def draw_expert_ids(key, part):
    group_scores = jax.random.randint(jax.random.fold_in(key, 101), (N_GRP, GROUPS), 0, 1 << 20) * GROUPS + jnp.arange(GROUPS, dtype=jnp.int32)[None, :]
    group_order = jnp.argsort(group_scores, axis=1).astype(jnp.int32)
    user_scores = jax.random.randint(jax.random.fold_in(key, 202), (N_GRP, GROUPS, USERS), 0, 1 << 20) * USERS + jnp.arange(USERS, dtype=jnp.int32)[None, None, :]
    user_order = jnp.argsort(user_scores, axis=2).astype(jnp.int32)
    member_scores = jax.random.randint(jax.random.fold_in(key, 303), (N_GRP, GROUPS, GROUP_EXP), 0, 1 << 20) * GROUP_EXP + jnp.arange(GROUP_EXP, dtype=jnp.int32)[None, None, :]
    member_order = jnp.argsort(member_scores, axis=2).astype(jnp.int32)
    ticket = TOPG * jnp.arange(ROWS_GRP, dtype=jnp.int32)[:, None] + jnp.arange(TOPG, dtype=jnp.int32)[None, :]
    position = ticket % GROUPS
    cycle_index = ticket // GROUPS
    blocks = jnp.arange(N_GRP, dtype=jnp.int32)[:, None, None]
    group_id = group_order[blocks, position[None, :, :]]
    user_slot = user_order[blocks, position[None, :, :], cycle_index[None, :, :]]
    pick_index = user_slot[:, :, :, None] + USERS * jnp.arange(PICK, dtype=jnp.int32)[None, None, None, :]
    member_rank = jnp.where(pick_index < CAP, 0, 1 + (pick_index - CAP) % (GROUP_EXP - 1))
    member = member_order[blocks[:, :, :, None], position[None, :, :, None], member_rank]
    experts = group_id[:, :, :, None] * GROUP_EXP + member
    return experts.reshape(TOKENS, TOPK).astype(jnp.int32)


def level_of(stream_key, extent, shards, low, top_value):
    loudness = 1.0
    for dim, blocks in shards:
        draws = jax.random.uniform(jax.random.fold_in(jax.random.fold_in(stream_key, 6), dim), (blocks,), jnp.float32, low / len(shards), top_value / len(shards))
        loudness = loudness * jnp.repeat(jnp.exp(draws), extent[dim] // blocks).reshape((-1,) + (1,) * (len(extent) - 1 - dim))
    return loudness


def bell_draw(key, shape, scale, reach, pieces=(), kind=jnp.bfloat16):
    entries = scale * jax.random.normal(key, shape, jnp.float32)
    if pieces:
        entries = entries * level_of(key, shape, pieces, -0.22, 0.18)
    return jnp.clip(entries, -reach, reach).astype(kind)


def setup_inputs(seed: int = 0) -> dict:
    key_list = jax.random.split(jax.random.key(seed), 7)
    return {
        "out_grad": bell_draw(key_list[0], (TOKENS, D), 1.0, 6.0, ((0, 8), (1, 4))),
        "expert_ids": draw_expert_ids(jax.random.fold_in(key_list[6], 71), 0),
        "router_logits": bell_draw(key_list[2], (TOKENS, EXPERTS), 1.0, 5.0, ((0, 8),), jnp.float32),
        "router_weight": bell_draw(key_list[3], (EXPERTS, D), D ** -0.5, 0.09375, ((1, 4),)),
        "expert_weight": bell_draw(key_list[4], (EXPERTS, D, FF), FF ** -0.5, 0.1875, ((0, 8), (1, 4))),
        "hidden_saved": bell_draw(key_list[5], (N_GRP, SLOTS, FF), 1.0, 6.0, ((0, 8),)),
    }


route_scale = 2.5


def slot_places(expert_ids):
    pair_rows = expert_ids.reshape(N_GRP, ROWS_GRP * TOPK)
    onehot = (pair_rows[:, :, None] == jnp.arange(EXPERTS, dtype=jnp.int32)[None, None, :]).astype(jnp.int32)
    pair_ranks = jnp.sum((jnp.cumsum(onehot, axis=1) - 1) * onehot, axis=2)
    source_block = jnp.arange(N_GRP, dtype=jnp.int32)[:, None]
    within = ((pair_rows % EXP_GRP) * N_GRP + source_block) * CAP + pair_ranks
    return ((pair_rows // EXP_GRP) * SLOTS + within).reshape(TOKENS * TOPK).astype(jnp.int32)


def reference(out_grad, expert_ids, router_logits, router_weight, expert_weight, hidden_saved):
    sig = jax.nn.sigmoid(router_logits.astype(jnp.float32))
    chosen = jnp.take_along_axis(sig, expert_ids, axis=1)
    route_probs = route_scale * chosen / jnp.sum(chosen, axis=1, keepdims=True)
    places = slot_places(expert_ids)
    pair_token = (jnp.arange(TOKENS * TOPK, dtype=jnp.int32) // TOPK).astype(jnp.int32)
    token_of_slot = jnp.zeros((N_GRP * SLOTS,), jnp.int32).at[places].set(pair_token)
    used_slot = jnp.zeros((N_GRP * SLOTS,), jnp.int32).at[places].set(jnp.ones((TOKENS * TOPK,), jnp.int32))
    slot_prob = jnp.zeros((N_GRP * SLOTS,), jnp.float32).at[places].set(route_probs.reshape(TOKENS * TOPK)).astype(jnp.bfloat16)
    span = N_GRP * CAP
    width = D // N_EP

    def owner_work(items):
        token_index, used_flag, prob_row, saved_rows, weights = items
        slot_rows = jnp.where(used_flag[:, None] > 0, out_grad[token_index], jnp.zeros((), jnp.bfloat16))
        grouped = slot_rows.reshape(EXP_GRP, span, N_EP, width).astype(jnp.float32)
        split_weights = weights.reshape(EXP_GRP, N_EP, width, FF).astype(jnp.float32)
        partial_sums = jnp.einsum("lmkd,lkdf->lkmf", grouped, split_weights)
        rounded = lax.optimization_barrier(partial_sums.astype(jnp.bfloat16)).astype(jnp.float32)
        summed = jnp.sum(rounded, axis=1).reshape(SLOTS, FF)
        prob_value = prob_row.astype(jnp.float32)
        hidden_grad = (prob_value[:, None] * summed).astype(jnp.bfloat16)
        slot_score = jnp.sum(saved_rows.astype(jnp.float32) * summed, axis=1)
        scaled_rows = (prob_value[:, None] * slot_rows.astype(jnp.float32)).astype(jnp.bfloat16)
        weight_grad = jnp.einsum(
            "lmd,lmf->ldf",
            scaled_rows.reshape(EXP_GRP, span, D).astype(jnp.float32),
            saved_rows.reshape(EXP_GRP, span, FF).astype(jnp.float32),
        ).astype(jnp.bfloat16)
        return weight_grad, hidden_grad, slot_score

    weight_grad, hidden_grad, slot_score = lax.map(
        owner_work,
        (
            token_of_slot.reshape(N_GRP, SLOTS),
            used_slot.reshape(N_GRP, SLOTS),
            slot_prob.reshape(N_GRP, SLOTS),
            hidden_saved,
            expert_weight.reshape(N_GRP, EXP_GRP, D, FF),
        ),
    )
    pair_score = slot_score.reshape(N_GRP * SLOTS)[places].reshape(TOKENS, TOPK)
    weighted_mean = jnp.sum(route_probs * pair_score, axis=1, keepdims=True) / route_scale
    logit_terms = route_probs * (1.0 - chosen) * (pair_score - weighted_mean)
    picked = expert_ids[:, :, None] == jnp.arange(EXPERTS, dtype=jnp.int32)[None, None, :]
    router_grad = jnp.sum(jnp.where(picked, logit_terms[:, :, None], jnp.zeros((), jnp.float32)), axis=1).astype(jnp.bfloat16)
    input_grad = jnp.dot(router_grad, router_weight, preferred_element_type=jnp.float32).astype(jnp.bfloat16)
    return weight_grad.reshape(EXPERTS, D, FF), hidden_grad, input_grad
```

```python
import jax
import jax.numpy as jnp
from jax import lax
from jax.sharding import PartitionSpec as P

route_scale = 2.5
LANES = 128


def slot_plan(out_grad, expert_ids, router_logits, router_weight, expert_weight, hidden_saved):
    group_rows, features = out_grad.shape
    top_count = expert_ids.shape[1]
    experts = router_logits.shape[1]
    group_count = lax.axis_size("grp")
    local_experts = expert_weight.shape[0]
    hidden_width = expert_weight.shape[2]
    slot_count = hidden_saved.shape[1]
    capacity = slot_count // (local_experts * group_count)
    expert_span = group_count * capacity
    pair_count = group_rows * top_count
    sig_values = jax.nn.sigmoid(router_logits)
    picked = expert_ids[:, :, None] == jnp.arange(experts, dtype=jnp.int32)[None, None, :]
    chosen = jnp.sum(jnp.where(picked, sig_values[:, None, :], 0.0), axis=2)
    route_probs = route_scale * chosen / jnp.sum(chosen, axis=1, keepdims=True)
    flat_ids = expert_ids.reshape(pair_count)
    onehot = picked.reshape(pair_count, experts).astype(jnp.int32)
    pair_ranks = jnp.sum((jnp.cumsum(onehot, axis=0) - 1) * onehot, axis=1)
    slot_place = (
        flat_ids % local_experts * group_count + flat_ids // local_experts
    ) * capacity + pair_ranks
    slot_match = slot_place[None, :] == jnp.arange(slot_count, dtype=jnp.int32)[:, None]
    token_pick = jnp.sum(
        slot_match.reshape(slot_count, group_rows, top_count).astype(jnp.float32), axis=2
    ).astype(jnp.bfloat16)
    send_rows = jnp.dot(token_pick, out_grad, preferred_element_type=jnp.float32).astype(
        jnp.bfloat16
    )
    send_prob = jnp.sum(
        jnp.where(slot_match, route_probs.reshape(1, pair_count), 0.0), axis=1
    ).astype(jnp.bfloat16)
    swap = dict(split_axis=1, concat_axis=1, tiled=True)
    shape = (local_experts, group_count, capacity)
    got_rows = lax.all_to_all(send_rows.reshape(shape + (features,)), "grp", **swap)
    got_prob = lax.all_to_all(send_prob.reshape(shape), "grp", **swap)
    slot_grads = got_rows.reshape(local_experts, expert_span, features)
    prob_rows = got_prob.reshape(local_experts, expert_span).astype(jnp.float32)
    saved_rows = hidden_saved.reshape(local_experts, expert_span, hidden_width)
    scaled_rows = (prob_rows[:, :, None] * slot_grads.astype(jnp.float32)).astype(jnp.bfloat16)
    weight_grad = jnp.einsum(
        "lmd,lmf->ldf", scaled_rows, saved_rows, preferred_element_type=jnp.float32
    ).astype(jnp.bfloat16)
    owner_index = lax.axis_index("ep")
    share_rows = slot_count // lax.axis_size("ep")
    flat_prob = prob_rows.reshape(slot_count)
    flat_saved = hidden_saved.reshape(slot_count, hidden_width)
    partial_term = jnp.einsum(
        "lmd,ldf->lmf", slot_grads, expert_weight, preferred_element_type=jnp.float32
    ).reshape(slot_count, hidden_width)
    rounded_term = lax.optimization_barrier(partial_term.astype(jnp.bfloat16)).astype(jnp.float32)
    partial_score = jnp.sum(flat_saved.astype(jnp.float32) * rounded_term, axis=1)
    moved_scores = lax.all_to_all(partial_score.reshape(shape), "grp", **swap)
    returned = lax.psum(moved_scores, "ep")
    summed = lax.psum_scatter(
        partial_term.astype(jnp.bfloat16), "ep", scatter_dimension=0, tiled=True
    ).astype(jnp.float32)
    own_prob = lax.dynamic_slice_in_dim(flat_prob, owner_index * share_rows, share_rows, 0)
    hidden_grad = (own_prob[:, None] * summed).astype(jnp.bfloat16)[None]
    pair_score = jnp.sum(
        jnp.where(slot_match, returned.reshape(slot_count, 1), 0.0), axis=0
    ).reshape(group_rows, top_count)
    weighted_mean = jnp.sum(route_probs * pair_score, axis=1, keepdims=True) / route_scale
    logit_terms = route_probs * (1.0 - chosen) * (pair_score - weighted_mean)
    router_grad = jnp.sum(jnp.where(picked, logit_terms[:, :, None], 0.0), axis=1).astype(
        jnp.bfloat16
    )
    input_grad = jnp.dot(router_grad, router_weight, preferred_element_type=jnp.float32).astype(
        jnp.bfloat16
    )
    return (weight_grad, hidden_grad, input_grad)


def exchange(x, distance):
    count = lax.axis_size("grp")
    return lax.ppermute(x, "grp", [(i, i ^ distance) for i in range(count)])


def gather_blocks(x):
    count = lax.axis_size("grp")
    blocks = {0: x}
    far = sorted(range(2, count, 2), key=lambda d: (d != count // 2, -d))
    for distance in far:
        blocks[distance] = exchange(x, distance)
    for distance in [0] + far:
        blocks[distance ^ 1] = exchange(blocks[distance], 1)
    return [blocks[d] for d in range(count)]


def token_plan(out_grad, expert_ids, router_logits, router_weight, expert_weight, hidden_saved):
    group_rows, features = out_grad.shape
    experts = router_logits.shape[1]
    group_count, ep_count = lax.axis_size("grp"), lax.axis_size("ep")
    local_experts, _, hidden_width = expert_weight.shape
    slot_count = hidden_saved.shape[1]
    capacity = slot_count // (local_experts * group_count)
    expert_span = group_count * capacity
    token_count = group_count * group_rows
    own_group, own_ep = lax.axis_index("grp"), lax.axis_index("ep")

    sig = jax.nn.sigmoid(router_logits).T
    named = jnp.any(
        expert_ids.T[None] == jnp.arange(experts, dtype=jnp.int32)[:, None, None], axis=1
    )
    chosen = jnp.where(named, sig, 0.0)
    probs = route_scale * chosen / jnp.sum(chosen, axis=0, keepdims=True)
    upto = jnp.arange(group_rows)[:, None] <= jnp.arange(group_rows)[None, :]
    ranks = jnp.dot(
        named.astype(jnp.bfloat16), upto.astype(jnp.bfloat16), preferred_element_type=jnp.float32
    )
    ranks = jnp.where(named, ranks, 0.0)

    pad = -2 * experts % LANES
    packed = jnp.concatenate(
        [
            out_grad,
            probs.T.astype(jnp.bfloat16),
            ranks.T.astype(jnp.bfloat16),
            jnp.zeros((group_rows, pad), jnp.bfloat16),
        ],
        axis=1,
    )
    blocks = gather_blocks(packed)
    rows = jnp.concatenate([b[:, :features] for b in blocks], axis=0)
    aux = jnp.concatenate([b[:, features:] for b in blocks], axis=0)
    own_experts = own_group * local_experts
    slot_probs = lax.dynamic_slice_in_dim(aux, own_experts, local_experts, 1).T
    slot_ranks = lax.dynamic_slice_in_dim(aux, experts + own_experts, local_experts, 1).T
    source = (jnp.arange(token_count, dtype=jnp.int32) // group_rows) ^ own_group
    place = jnp.where(
        slot_ranks > 0, source[None] * capacity + slot_ranks.astype(jnp.int32) - 1, -1
    )
    pick = place[:, None, :] == jnp.arange(expert_span, dtype=jnp.int32)[None, :, None]
    pick_rows = pick.astype(jnp.bfloat16)
    slot_grads = jnp.einsum(
        "lmt,td->lmd", pick_rows, rows, preferred_element_type=jnp.float32
    ).astype(jnp.bfloat16)
    prob_rows = jnp.sum(jnp.where(pick, slot_probs[:, None, :].astype(jnp.float32), 0.0), axis=2)
    saved_rows = hidden_saved.reshape(local_experts, expert_span, hidden_width)
    partial_term = jnp.einsum(
        "lmd,ldf->lmf", slot_grads, expert_weight, preferred_element_type=jnp.float32
    ).astype(jnp.bfloat16)
    partial_term = lax.optimization_barrier(partial_term)
    partial_score = jnp.sum(
        saved_rows.astype(jnp.float32) * partial_term.astype(jnp.float32), axis=2
    )
    to_blocks = partial_score.reshape(local_experts, group_count, capacity).transpose(1, 0, 2)
    to_all = jnp.broadcast_to(
        to_blocks[:, None], (group_count, ep_count, local_experts, capacity)
    ).reshape(group_count * ep_count, local_experts * capacity)
    from_all = lax.all_to_all(to_all, ("grp", "ep"), 0, 0, tiled=True)

    scaled_rows = (prob_rows[:, :, None] * slot_grads.astype(jnp.float32)).astype(jnp.bfloat16)
    weight_grad = jnp.einsum(
        "lmd,lmf->ldf", scaled_rows, saved_rows, preferred_element_type=jnp.float32
    ).astype(jnp.bfloat16)

    share_rows = slot_count // ep_count
    held = partial_term.reshape(1, slot_count, hidden_width)
    bit = 1
    piece = partial_term.reshape(ep_count, share_rows, hidden_width)
    while bit < ep_count:
        pairs = [(i, i ^ bit) for i in range(ep_count)]
        left = piece.shape[0] // 2
        own_bit = (own_ep // bit) % 2
        halves = piece.reshape(left, 2, share_rows, hidden_width)
        keep = lax.dynamic_index_in_dim(halves, own_bit, 1, False)
        send = lax.dynamic_index_in_dim(halves, 1 - own_bit, 1, False)
        got = lax.ppermute(send, "ep", pairs)
        total = keep.astype(jnp.float32) + got.astype(jnp.float32)
        piece = total.astype(jnp.bfloat16) if left > 1 else total
        bit *= 2
    summed = piece.reshape(share_rows, hidden_width)
    own_prob = lax.dynamic_slice_in_dim(
        prob_rows.reshape(slot_count), own_ep * share_rows, share_rows, 0
    )
    hidden_grad = (own_prob[:, None] * summed).astype(jnp.bfloat16)[None]

    returned = jnp.sum(
        from_all.reshape(group_count, ep_count, local_experts, capacity), axis=1
    ).reshape(experts, capacity)
    at_rank = ranks[:, None, :] == jnp.arange(1, capacity + 1, dtype=jnp.float32)[None, :, None]
    scores = jnp.sum(jnp.where(at_rank, returned[:, :, None], 0.0), axis=1)
    mean = jnp.sum(probs * scores, axis=0, keepdims=True) / route_scale
    router_grad = jnp.where(named, probs * (1.0 - sig) * (scores - mean), 0.0).astype(jnp.bfloat16)
    input_grad = lax.dot_general(
        router_grad, router_weight, (((0,), (0,)), ((), ())), preferred_element_type=jnp.float32
    ).astype(jnp.bfloat16)
    return (weight_grad, hidden_grad, input_grad)


def body(out_grad, expert_ids, router_logits, router_weight, expert_weight, hidden_saved):
    group_count, ep_count = lax.axis_size("grp"), lax.axis_size("ep")
    tokens = out_grad.shape[0] * group_count
    slots = hidden_saved.shape[1]
    powers = group_count & (group_count - 1) == 0 and ep_count & (ep_count - 1) == 0
    plan = token_plan if tokens <= slots and powers else slot_plan
    return plan(
        out_grad, expert_ids, router_logits, router_weight, expert_weight, hidden_saved
    )


def solution(mesh):
    in_specs = (
        P("grp", "ep"),
        P("grp", None),
        P("grp", None),
        P(None, "ep"),
        P("grp", "ep", None),
        P("grp", None, None),
    )
    out_specs = (P("grp", "ep", None), P("grp", "ep", None), P("grp", "ep"))
    return jax.shard_map(body, mesh=mesh, in_specs=in_specs, out_specs=out_specs, check_vma=False)
```

```python
import functools

import jax
import jax.numpy as jnp
from jax import lax
from jax.experimental import pallas as pl
from jax.experimental.pallas import tpu as pltpu
from jax.sharding import PartitionSpec as P


route_scale = 2.5
LANES = 128


def slot_plan(out_grad, expert_ids, router_logits, router_weight, expert_weight, hidden_saved):
    group_rows, features = out_grad.shape
    top_count = expert_ids.shape[1]
    experts = router_logits.shape[1]
    group_count = lax.axis_size("grp")
    local_experts = expert_weight.shape[0]
    hidden_width = expert_weight.shape[2]
    slot_count = hidden_saved.shape[1]
    capacity = slot_count // (local_experts * group_count)
    expert_span = group_count * capacity
    pair_count = group_rows * top_count
    sig_values = jax.nn.sigmoid(router_logits)
    picked = expert_ids[:, :, None] == jnp.arange(experts, dtype=jnp.int32)[None, None, :]
    chosen = jnp.sum(jnp.where(picked, sig_values[:, None, :], 0.0), axis=2)
    route_probs = route_scale * chosen / jnp.sum(chosen, axis=1, keepdims=True)
    flat_ids = expert_ids.reshape(pair_count)
    onehot = picked.reshape(pair_count, experts).astype(jnp.int32)
    pair_ranks = jnp.sum((jnp.cumsum(onehot, axis=0) - 1) * onehot, axis=1)
    slot_place = (
        flat_ids % local_experts * group_count + flat_ids // local_experts
    ) * capacity + pair_ranks
    slot_match = slot_place[None, :] == jnp.arange(slot_count, dtype=jnp.int32)[:, None]
    token_pick = jnp.sum(
        slot_match.reshape(slot_count, group_rows, top_count).astype(jnp.float32), axis=2
    ).astype(jnp.bfloat16)
    send_rows = jnp.dot(token_pick, out_grad, preferred_element_type=jnp.float32).astype(
        jnp.bfloat16
    )
    send_prob = jnp.sum(
        jnp.where(slot_match, route_probs.reshape(1, pair_count), 0.0), axis=1
    ).astype(jnp.bfloat16)
    swap = dict(split_axis=1, concat_axis=1, tiled=True)
    shape = (local_experts, group_count, capacity)
    got_rows = lax.all_to_all(send_rows.reshape(shape + (features,)), "grp", **swap)
    got_prob = lax.all_to_all(send_prob.reshape(shape), "grp", **swap)
    slot_grads = got_rows.reshape(local_experts, expert_span, features)
    prob_rows = got_prob.reshape(local_experts, expert_span).astype(jnp.float32)
    saved_rows = hidden_saved.reshape(local_experts, expert_span, hidden_width)
    scaled_rows = (prob_rows[:, :, None] * slot_grads.astype(jnp.float32)).astype(jnp.bfloat16)
    weight_grad = jnp.einsum(
        "lmd,lmf->ldf", scaled_rows, saved_rows, preferred_element_type=jnp.float32
    ).astype(jnp.bfloat16)
    owner_index = lax.axis_index("ep")
    share_rows = slot_count // lax.axis_size("ep")
    flat_prob = prob_rows.reshape(slot_count)
    flat_saved = hidden_saved.reshape(slot_count, hidden_width)
    partial_term = jnp.einsum(
        "lmd,ldf->lmf", slot_grads, expert_weight, preferred_element_type=jnp.float32
    ).reshape(slot_count, hidden_width)
    rounded_term = lax.optimization_barrier(partial_term.astype(jnp.bfloat16)).astype(jnp.float32)
    partial_score = jnp.sum(flat_saved.astype(jnp.float32) * rounded_term, axis=1)
    moved_scores = lax.all_to_all(partial_score.reshape(shape), "grp", **swap)
    returned = lax.psum(moved_scores, "ep")
    summed = lax.psum_scatter(
        partial_term.astype(jnp.bfloat16), "ep", scatter_dimension=0, tiled=True
    ).astype(jnp.float32)
    own_prob = lax.dynamic_slice_in_dim(flat_prob, owner_index * share_rows, share_rows, 0)
    hidden_grad = (own_prob[:, None] * summed).astype(jnp.bfloat16)[None]
    pair_score = jnp.sum(
        jnp.where(slot_match, returned.reshape(slot_count, 1), 0.0), axis=0
    ).reshape(group_rows, top_count)
    weighted_mean = jnp.sum(route_probs * pair_score, axis=1, keepdims=True) / route_scale
    logit_terms = route_probs * (1.0 - chosen) * (pair_score - weighted_mean)
    router_grad = jnp.sum(jnp.where(picked, logit_terms[:, :, None], 0.0), axis=1).astype(
        jnp.bfloat16
    )
    input_grad = jnp.dot(router_grad, router_weight, preferred_element_type=jnp.float32).astype(
        jnp.bfloat16
    )
    return (weight_grad, hidden_grad, input_grad)


def exchange(x, distance):
    count = lax.axis_size("grp")
    return lax.ppermute(x, "grp", [(i, i ^ distance) for i in range(count)])


def gather_blocks(x):
    count = lax.axis_size("grp")
    blocks = {0: x}
    far = sorted(range(2, count, 2), key=lambda d: (d != count // 2, -d))
    for distance in far:
        blocks[distance] = exchange(x, distance)
    for distance in [0] + far:
        blocks[distance ^ 1] = exchange(blocks[distance], 1)
    return [blocks[d] for d in range(count)]


def iota(shape, dim):
    return lax.broadcasted_iota(jnp.int32, shape, dim)


def contract_rows(a, b):
    return lax.dot_general(a, b, (((0,), (0,)), ((), ())), preferred_element_type=jnp.float32)


def pack_kernel(local, ids_hbm, logits_hbm, rows_hbm, packed_ref, meta_ref, ids_ref, logits_ref, sems):
    top_count, tokens = ids_ref.shape
    groups = logits_ref.shape[0] // local
    features = rows_hbm.shape[1]
    copies = [
        pltpu.make_async_copy(ids_hbm, ids_ref, sems.at[0]),
        pltpu.make_async_copy(logits_hbm, logits_ref, sems.at[1]),
        pltpu.make_async_copy(rows_hbm, packed_ref.at[:, pl.ds(0, features)], sems.at[2]),
    ]
    for c in copies:
        c.start()
    copies[0].wait()
    copies[1].wait()
    ids = ids_ref[...]
    upto = (iota((tokens, tokens), 0) <= iota((tokens, tokens), 1)).astype(jnp.bfloat16)
    sig, chosen, ranks = [], [], []
    for l in range(local):
        expert = iota((groups, tokens), 0) * local + l
        hit = jnp.zeros((groups, tokens), jnp.float32)
        for i in range(top_count):
            hit = hit + (ids[i : i + 1, :] == expert).astype(jnp.float32)
        value = jax.nn.sigmoid(logits_ref[pl.ds(l, groups, stride=local), :])
        sig.append(value)
        chosen.append(hit * value)
        count = jnp.dot(hit.astype(jnp.bfloat16), upto, preferred_element_type=jnp.float32)
        ranks.append(hit * count)
    total = sum(jnp.sum(c, axis=0, keepdims=True) for c in chosen)
    probs = [route_scale * c / total for c in chosen]
    stack = jnp.concatenate(probs + ranks, axis=0).astype(jnp.bfloat16)
    lanes = packed_ref.shape[1] - features
    spread = (iota((stack.shape[0], lanes), 0) == iota((stack.shape[0], lanes), 1)).astype(
        jnp.bfloat16
    )
    packed_ref[:, features:] = contract_rows(stack, spread).astype(jnp.bfloat16)
    for l in range(local):
        for k, value in enumerate((sig[l], probs[l], ranks[l])):
            meta_ref[l, k] = jnp.zeros(meta_ref.shape[2:], jnp.float32)
            meta_ref[l, k, :, :tokens] = value
    copies[2].wait()


def load_kernel(parts, cue_ref, w_ref, h_ref, r_ref, w_out, h_out, r_out, sems):
    rows = w_ref.shape[1] // parts
    copies = [
        pltpu.make_async_copy(
            w_ref.at[l, pl.ds(i * rows, rows)],
            w_out.at[l, pl.ds(i * rows, rows)],
            sems.at[l * parts + i],
        )
        for l in range(w_ref.shape[0])
        for i in range(parts)
    ]
    base = w_ref.shape[0] * parts
    copies.append(pltpu.make_async_copy(h_ref, h_out, sems.at[base]))
    copies.append(pltpu.make_async_copy(r_ref, r_out, sems.at[base + 1]))
    for c in copies:
        c.start()
    for c in copies:
        c.wait()


def partial_kernel(local, groups, capacity, *refs):
    blocks = refs[:groups]
    w_ref, h_ref, keep_ref, send_ref, score_ref = refs[groups:]
    features, width = w_ref.shape[1], w_ref.shape[2]
    span = groups * capacity
    tokens = groups * blocks[0].shape[0]
    cols = 256 if width % 256 == 0 else LANES
    own, half = lax.axis_index("grp"), lax.rem(lax.axis_index("ep"), 2)
    rows = jnp.concatenate([b[:, :features] for b in blocks], axis=0)
    aux = jnp.concatenate([b[:, features:] for b in blocks], axis=0).astype(jnp.float32)
    aux = aux.T
    source = (iota((1, tokens), 1) // blocks[0].shape[0]) ^ own
    slot = iota((span, tokens), 0) + half * (span // 2)
    slot = jnp.where(slot >= span, slot - span, slot)
    part_row, part_lane = iota((span, LANES), 0), iota((span, LANES), 1)
    near = pl.ds(pl.multiple_of(half * (span // 2), span // 2), span // 2)
    away = pl.ds(pl.multiple_of((1 - half) * (span // 2), span // 2), span // 2)
    sent = jnp.zeros((groups, LANES), jnp.float32)
    for l in range(local):
        lane = l * groups + own
        prob = jnp.sum(jnp.where(iota(aux.shape, 0) == lane, aux, 0.0), axis=0, keepdims=True)
        rank = jnp.sum(
            jnp.where(iota(aux.shape, 0) == local * groups + lane, aux, 0.0),
            axis=0,
            keepdims=True,
        ).astype(jnp.int32)
        place = jnp.where(rank > 0, source * capacity + rank - 1, -1)
        pick = slot == place
        scale = jnp.sum(jnp.where(pick, prob, 0.0), axis=1, keepdims=True)
        grads = jnp.dot(
            pick.astype(jnp.float32).astype(jnp.bfloat16), rows, preferred_element_type=jnp.float32
        ).astype(jnp.bfloat16)
        score = jnp.zeros((span, LANES), jnp.float32)
        for n in range(width // cols):
            part = pl.ds(n * cols, cols)
            term = jnp.dot(grads, w_ref[l, :, part], preferred_element_type=jnp.float32)
            saved = jnp.concatenate([h_ref[l, near, part], h_ref[l, away, part]], axis=0)
            product = term * saved.astype(jnp.float32)
            for k in range(cols // LANES):
                score = score + product[:, k * LANES : (k + 1) * LANES]
            out = (term * scale).astype(jnp.bfloat16)
            keep_ref[l, :, part] = out[: span // 2]
            send_ref[l, :, part] = out[span // 2 :]
        score = jnp.sum(score, axis=1, keepdims=True)
        spread = jnp.where(lax.rem(part_row, capacity) + l * capacity == part_lane, score, 0.0)
        sent = sent + jnp.sum(spread.reshape(groups, capacity, LANES), axis=1)
    turned = jnp.concatenate([sent[groups // 2 :], sent[: groups // 2]], axis=0)
    sent = jnp.where(half == 0, sent, turned)
    score_ref[...] = jnp.broadcast_to(sent[:, None, :], score_ref.shape)


def weight_kernel(local, groups, capacity, parts, *refs):
    blocks = refs[:groups]
    h_ref, out_hbm, turned_buf, scaled_buf, out_buf, sems = refs[groups:]
    features = turned_buf.shape[0]
    tile = features // parts
    block_rows = blocks[0].shape[0]
    span = groups * capacity
    tokens = groups * block_rows
    own = lax.axis_index("grp")
    rows = jnp.concatenate([b[:, :features] for b in blocks], axis=0)
    turned_buf[...] = rows.T
    aux = jnp.concatenate([b[:, features:] for b in blocks], axis=0).astype(jnp.float32)
    at = iota(aux.shape, 1)
    source = (iota((tokens, 1), 0) // block_rows) ^ own
    copies = []
    for l in range(local):
        lane = l * groups + own
        prob = jnp.sum(jnp.where(at == lane, aux, 0.0), axis=1, keepdims=True)
        rank = jnp.sum(jnp.where(at == local * groups + lane, aux, 0.0), axis=1, keepdims=True)
        place = jnp.where(rank > 0, source * capacity + rank.astype(jnp.int32) - 1, -1)
        pick = jnp.where(place == iota((tokens, span), 1), prob, 0.0).astype(jnp.bfloat16)
        scaled_buf[...] = jnp.dot(
            turned_buf[...], pick, preferred_element_type=jnp.float32
        ).astype(jnp.bfloat16)
        for d in range(parts):
            part = pl.ds(d * tile, tile)
            out_buf[l, part] = jnp.dot(
                scaled_buf[part], h_ref[l], preferred_element_type=jnp.float32
            ).astype(jnp.bfloat16)
            copy = pltpu.make_async_copy(
                out_buf.at[l, part], out_hbm.at[l, part], sems.at[l * parts + d]
            )
            copy.start()
            copies.append(copy)
    for copy in copies:
        copy.wait()


def pair_kernel(mine_ref, got_ref, keep_ref, send_ref):
    bit = lax.axis_index("ep") // 2
    keep_ref[...] = mine_ref[bit].astype(jnp.float32) + got_ref[bit].astype(jnp.float32)
    send_ref[...] = (
        mine_ref[1 - bit].astype(jnp.float32) + got_ref[1 - bit].astype(jnp.float32)
    ).astype(jnp.bfloat16)


def router_kernel(local, capacity, score_ref, meta_ref, w_ref, out_ref):
    groups, tokens = meta_ref.shape[2], out_ref.shape[0]
    found = jnp.sum(score_ref[...], axis=1)
    scores = []
    for l in range(local):
        rank = meta_ref[l, 2].astype(jnp.int32)
        at = jnp.maximum(rank + (l * capacity - 1), 0)
        value = jnp.take_along_axis(found, at, axis=1, mode="promise_in_bounds")
        scores.append(jnp.where(rank > 0, value, 0.0))
    mean = sum(
        jnp.sum(meta_ref[l, 1] * scores[l], axis=0, keepdims=True) for l in range(local)
    ) * (1.0 / route_scale)
    grads = jnp.concatenate(
        [
            meta_ref[l, 1] * (1.0 - meta_ref[l, 0]) * (scores[l] - mean)
            for l in range(local)
        ],
        axis=0,
    ).astype(jnp.bfloat16)
    count = local * groups
    row = iota((count, count), 0)
    expert = lax.rem(row, groups) * local + row // groups
    order = (expert == iota((count, count), 1)).astype(jnp.bfloat16)
    turned = contract_rows(grads, order)[:tokens].astype(jnp.bfloat16)
    out_ref[...] = jnp.dot(turned, w_ref[...], preferred_element_type=jnp.float32).astype(
        jnp.bfloat16
    )


def cost(flops, nbytes):
    return pl.CostEstimate(flops=flops, bytes_accessed=nbytes, transcendentals=0)


def struct(shape, dtype):
    return jax.ShapeDtypeStruct(shape, dtype)


def held(x):
    return pltpu.with_memory_space_constraint(x, pltpu.VMEM)


def away_from_vmem(x):
    return pltpu.with_memory_space_constraint(x, pltpu.HBM)


def kept(shape, dtype):
    return pltpu.VMEM(shape, dtype)


def token_plan(out_grad, expert_ids, router_logits, router_weight, expert_weight, hidden_saved):
    group_rows, features = out_grad.shape
    groups, ep_count = lax.axis_size("grp"), lax.axis_size("ep")
    local, _, width = expert_weight.shape
    slot_count = hidden_saved.shape[1]
    capacity = slot_count // (local * groups)
    span = groups * capacity
    tokens = groups * group_rows
    bf16, f32 = jnp.bfloat16, jnp.float32
    vmem = pl.BlockSpec(memory_space=pltpu.VMEM)
    hbm = pl.BlockSpec(memory_space=pltpu.HBM)

    def limit(mib):
        return pltpu.CompilerParams(vmem_limit_bytes=mib * 2**20)

    packed, meta = pl.pallas_call(
        functools.partial(pack_kernel, local),
        out_shape=(
            pltpu.VMEM((group_rows, features + LANES), bf16),
            pltpu.VMEM((local, 3, groups, LANES), f32),
        ),
        in_specs=[hbm] * 3,
        out_specs=(vmem, vmem),
        scratch_shapes=[
            pltpu.VMEM(expert_ids.shape[::-1], jnp.int32),
            pltpu.VMEM(router_logits.shape[::-1], f32),
            pltpu.SemaphoreType.DMA((3,)),
        ],
        compiler_params=limit(2),
        name="pack",
    )(away_from_vmem(expert_ids.T), away_from_vmem(router_logits.T), away_from_vmem(out_grad))
    blocks = [held(b) for b in gather_blocks(packed)]

    weights, saved, projection = pl.pallas_call(
        functools.partial(load_kernel, 2),
        out_shape=(
            pltpu.VMEM(expert_weight.shape, bf16),
            pltpu.VMEM((local, span, width), bf16),
            pltpu.VMEM(router_weight.shape, bf16),
        ),
        in_specs=[vmem] + [hbm] * 3,
        out_specs=(vmem, vmem, vmem),
        scratch_shapes=[pltpu.SemaphoreType.DMA((2 * local + 2,))],
        compiler_params=limit(2),
        cost_estimate=cost(2**27, 8 * 2**20),
        name="load",
    )(
        blocks[2],
        away_from_vmem(expert_weight),
        away_from_vmem(hidden_saved.reshape(local, span, width)),
        away_from_vmem(router_weight),
    )
    weights, saved, projection = held(weights), held(saved), held(projection)

    keep, send, score = pl.pallas_call(
        functools.partial(partial_kernel, local, groups, capacity),
        out_shape=(
            pltpu.VMEM((local, span // 2, width), bf16),
            pltpu.VMEM((local, span // 2, width), bf16),
            pltpu.VMEM((groups, ep_count, LANES), f32),
        ),
        in_specs=[vmem] * (groups + 2),
        out_specs=(vmem, vmem, vmem),
        compiler_params=limit(8),
        cost_estimate=cost(2 * slot_count * features * width, 8 * 2**20),
        name="partial",
    )(*blocks, weights, saved)

    core_pairs = [(i, i ^ 1) for i in range(ep_count)]
    chip_pairs = [(i, i ^ 2) for i in range(ep_count)]
    got = lax.ppermute(send, "ep", core_pairs)
    from_all = lax.all_to_all(
        score.reshape(groups * ep_count, 1, LANES), ("grp", "ep"), 0, 0, tiled=True
    )
    mine, away = pl.pallas_call(
        pair_kernel,
        out_shape=(kept((span // 2, width), f32), kept((span // 2, width), bf16)),
        in_specs=[vmem, vmem],
        out_specs=(vmem, vmem),
        compiler_params=limit(2),
        name="pair",
    )(held(keep), held(got))
    last = lax.ppermute(away, "ep", chip_pairs)

    parts = 4
    weight_grad = pl.pallas_call(
        functools.partial(weight_kernel, local, groups, capacity, parts),
        out_shape=struct((local, features, width), bf16),
        in_specs=[vmem] * (groups + 1),
        out_specs=hbm,
        scratch_shapes=[
            pltpu.VMEM((features, tokens), bf16),
            pltpu.VMEM((features, span), bf16),
            pltpu.VMEM((local, features, width), bf16),
            pltpu.SemaphoreType.DMA((local * parts,)),
        ],
        compiler_params=limit(12),
        cost_estimate=cost(2 * slot_count * features * width, 6 * 2**20),
        name="weight",
    )(*blocks, saved)

    hidden_grad = (mine + last.astype(f32)).astype(bf16)[None]

    input_grad = pl.pallas_call(
        functools.partial(router_kernel, local, capacity),
        out_shape=struct((group_rows, features), bf16),
        in_specs=[vmem] * 3,
        out_specs=vmem,
        compiler_params=limit(2),
        name="router",
    )(held(from_all.reshape(groups, ep_count, LANES)), held(meta), projection)
    return (weight_grad, hidden_grad, input_grad)


def body(out_grad, expert_ids, router_logits, router_weight, expert_weight, hidden_saved):
    groups, ep_count = lax.axis_size("grp"), lax.axis_size("ep")
    rows, experts = router_logits.shape
    slots = hidden_saved.shape[1]
    local = expert_weight.shape[0]
    fits = (
        rows * groups <= slots
        and groups % 8 == 0
        and groups & (groups - 1) == 0
        and (local, ep_count) == (2, 4)
        and rows % 16 == 0
        and slots // groups <= LANES
        and 2 * experts <= LANES
    )
    plan = token_plan if fits else slot_plan
    return plan(
        out_grad, expert_ids, router_logits, router_weight, expert_weight, hidden_saved
    )


def solution(mesh):
    in_specs = (
        P("grp", "ep"),
        P("grp", None),
        P("grp", None),
        P(None, "ep"),
        P("grp", "ep", None),
        P("grp", None, None),
    )
    out_specs = (P("grp", "ep", None), P("grp", "ep", None), P("grp", "ep"))
    return jax.shard_map(body, mesh=mesh, in_specs=in_specs, out_specs=out_specs, check_vma=False)
```

```python
import functools

import jax
import jax.numpy as jnp
from jax import lax
from jax.experimental import pallas as pl
from jax.experimental.pallas import tpu as pltpu
from jax.sharding import PartitionSpec as P


route_scale = 2.5
LANES = 128


def slot_plan(out_grad, expert_ids, router_logits, router_weight, expert_weight, hidden_saved):
    group_rows, features = out_grad.shape
    top_count = expert_ids.shape[1]
    experts = router_logits.shape[1]
    group_count = lax.axis_size("grp")
    local_experts = expert_weight.shape[0]
    hidden_width = expert_weight.shape[2]
    slot_count = hidden_saved.shape[1]
    capacity = slot_count // (local_experts * group_count)
    expert_span = group_count * capacity
    pair_count = group_rows * top_count
    sig_values = jax.nn.sigmoid(router_logits)
    picked = expert_ids[:, :, None] == jnp.arange(experts, dtype=jnp.int32)[None, None, :]
    chosen = jnp.sum(jnp.where(picked, sig_values[:, None, :], 0.0), axis=2)
    route_probs = route_scale * chosen / jnp.sum(chosen, axis=1, keepdims=True)
    flat_ids = expert_ids.reshape(pair_count)
    onehot = picked.reshape(pair_count, experts).astype(jnp.int32)
    pair_ranks = jnp.sum((jnp.cumsum(onehot, axis=0) - 1) * onehot, axis=1)
    slot_place = (
        flat_ids % local_experts * group_count + flat_ids // local_experts
    ) * capacity + pair_ranks
    slot_match = slot_place[None, :] == jnp.arange(slot_count, dtype=jnp.int32)[:, None]
    token_pick = jnp.sum(
        slot_match.reshape(slot_count, group_rows, top_count).astype(jnp.float32), axis=2
    ).astype(jnp.bfloat16)
    send_rows = jnp.dot(token_pick, out_grad, preferred_element_type=jnp.float32).astype(
        jnp.bfloat16
    )
    send_prob = jnp.sum(
        jnp.where(slot_match, route_probs.reshape(1, pair_count), 0.0), axis=1
    ).astype(jnp.bfloat16)
    swap = dict(split_axis=1, concat_axis=1, tiled=True)
    shape = (local_experts, group_count, capacity)
    got_rows = lax.all_to_all(send_rows.reshape(shape + (features,)), "grp", **swap)
    got_prob = lax.all_to_all(send_prob.reshape(shape), "grp", **swap)
    slot_grads = got_rows.reshape(local_experts, expert_span, features)
    prob_rows = got_prob.reshape(local_experts, expert_span).astype(jnp.float32)
    saved_rows = hidden_saved.reshape(local_experts, expert_span, hidden_width)
    scaled_rows = (prob_rows[:, :, None] * slot_grads.astype(jnp.float32)).astype(jnp.bfloat16)
    weight_grad = jnp.einsum(
        "lmd,lmf->ldf", scaled_rows, saved_rows, preferred_element_type=jnp.float32
    ).astype(jnp.bfloat16)
    owner_index = lax.axis_index("ep")
    share_rows = slot_count // lax.axis_size("ep")
    flat_prob = prob_rows.reshape(slot_count)
    flat_saved = hidden_saved.reshape(slot_count, hidden_width)
    partial_term = jnp.einsum(
        "lmd,ldf->lmf", slot_grads, expert_weight, preferred_element_type=jnp.float32
    ).reshape(slot_count, hidden_width)
    rounded_term = lax.optimization_barrier(partial_term.astype(jnp.bfloat16)).astype(jnp.float32)
    partial_score = jnp.sum(flat_saved.astype(jnp.float32) * rounded_term, axis=1)
    moved_scores = lax.all_to_all(partial_score.reshape(shape), "grp", **swap)
    returned = lax.psum(moved_scores, "ep")
    summed = lax.psum_scatter(
        partial_term.astype(jnp.bfloat16), "ep", scatter_dimension=0, tiled=True
    ).astype(jnp.float32)
    own_prob = lax.dynamic_slice_in_dim(flat_prob, owner_index * share_rows, share_rows, 0)
    hidden_grad = (own_prob[:, None] * summed).astype(jnp.bfloat16)[None]
    pair_score = jnp.sum(
        jnp.where(slot_match, returned.reshape(slot_count, 1), 0.0), axis=0
    ).reshape(group_rows, top_count)
    weighted_mean = jnp.sum(route_probs * pair_score, axis=1, keepdims=True) / route_scale
    logit_terms = route_probs * (1.0 - chosen) * (pair_score - weighted_mean)
    router_grad = jnp.sum(jnp.where(picked, logit_terms[:, :, None], 0.0), axis=1).astype(
        jnp.bfloat16
    )
    input_grad = jnp.dot(router_grad, router_weight, preferred_element_type=jnp.float32).astype(
        jnp.bfloat16
    )
    return (weight_grad, hidden_grad, input_grad)


def exchange(x, distance):
    count = lax.axis_size("grp")
    return lax.ppermute(x, "grp", [(i, i ^ distance) for i in range(count)])


def swap_order(count):
    top, rest = count - 2, list(range(2, count - 2, 2))
    return [top, 1] + rest + [top ^ 1, 3] + [d ^ 1 for d in rest if d != 2]


def gather_blocks(x):
    count = lax.axis_size("grp")
    blocks = {0: x}
    for distance in swap_order(count):
        if distance == 3:
            source, step = 1, 2
        else:
            source, step = (distance ^ 1, 1) if distance & 1 else (0, distance)
        blocks[distance] = exchange(blocks[source], step)
    return [blocks[d] for d in range(count)]


def iota(shape, dim):
    return lax.broadcasted_iota(jnp.int32, shape, dim)


def contract_rows(a, b):
    return lax.dot_general(a, b, (((0,), (0,)), ((), ())), preferred_element_type=jnp.float32)


def pack_kernel(local, ids_hbm, logits_hbm, rows_hbm, packed_ref, meta_ref, ids_ref, logits_ref, sems):
    top_count, tokens = ids_ref.shape
    groups = logits_ref.shape[0] // local
    features = rows_hbm.shape[1]
    copies = [
        pltpu.make_async_copy(ids_hbm, ids_ref, sems.at[0]),
        pltpu.make_async_copy(logits_hbm, logits_ref, sems.at[1]),
        pltpu.make_async_copy(rows_hbm, packed_ref.at[:, pl.ds(0, features)], sems.at[2]),
    ]
    for c in copies:
        c.start()
    copies[0].wait()
    copies[1].wait()
    ids = ids_ref[...]
    upto = (iota((tokens, tokens), 0) <= iota((tokens, tokens), 1)).astype(jnp.bfloat16)
    sig, chosen, ranks = [], [], []
    for l in range(local):
        expert = iota((groups, tokens), 0) * local + l
        hit = jnp.zeros((groups, tokens), jnp.float32)
        for i in range(top_count):
            hit = hit + (ids[i : i + 1, :] == expert).astype(jnp.float32)
        value = jax.nn.sigmoid(logits_ref[pl.ds(l, groups, stride=local), :])
        sig.append(value)
        chosen.append(hit * value)
        count = jnp.dot(hit.astype(jnp.bfloat16), upto, preferred_element_type=jnp.float32)
        ranks.append(hit * count)
    total = sum(jnp.sum(c, axis=0, keepdims=True) for c in chosen)
    probs = [route_scale * c / total for c in chosen]
    stack = jnp.concatenate(probs + ranks, axis=0).astype(jnp.bfloat16)
    lanes = packed_ref.shape[1] - features
    spread = (iota((stack.shape[0], lanes), 0) == iota((stack.shape[0], lanes), 1)).astype(
        jnp.bfloat16
    )
    packed_ref[:, features:] = contract_rows(stack, spread).astype(jnp.bfloat16)
    for l in range(local):
        for k, value in enumerate((sig[l], probs[l], ranks[l])):
            meta_ref[l, k] = jnp.zeros(meta_ref.shape[2:], jnp.float32)
            meta_ref[l, k, :, :tokens] = value
    copies[2].wait()


def half_of(parity, local, groups, capacity, blocks, saved_ref, weight, outs):
    keep_ref, send_ref = outs
    block_rows, features = blocks[0].shape[0], blocks[0].shape[1] - LANES
    width = keep_ref.shape[2]
    count = groups // 2
    span, tokens = count * capacity, count * block_rows
    cols = 256 if width % 256 == 0 else LANES
    own, side = lax.axis_index("grp"), lax.rem(lax.axis_index("ep"), 2)
    rows = jnp.concatenate([b[:, :features] for b in blocks], axis=0)
    aux = jnp.concatenate([b[:, features:] for b in blocks], axis=0).astype(jnp.float32).T
    source = (iota((1, tokens), 1) // block_rows) ^ (own // 2)
    slot = iota((span, tokens), 0) + side * (span // 2)
    slot = jnp.where(slot >= span, slot - span, slot)
    near = pl.ds(side * (count // 2), count // 2)
    away = pl.ds((1 - side) * (count // 2), count // 2)
    part_row, part_lane = iota((span, LANES), 0), iota((span, LANES), 1)
    sent = jnp.zeros((count, LANES), jnp.float32)
    for l in range(local):
        lane = l * groups + own
        row = iota(aux.shape, 0)
        prob = jnp.sum(jnp.where(row == lane, aux, 0.0), axis=0, keepdims=True)
        rank = jnp.sum(jnp.where(row == local * groups + lane, aux, 0.0), axis=0, keepdims=True)
        place = jnp.where(rank > 0, source * capacity + rank.astype(jnp.int32) - 1, -1)
        pick = slot == place
        scale = jnp.sum(jnp.where(pick, prob, 0.0), axis=1, keepdims=True)
        grads = jnp.dot(
            pick.astype(jnp.float32).astype(jnp.bfloat16), rows, preferred_element_type=jnp.float32
        ).astype(jnp.bfloat16)
        score = jnp.zeros((span, LANES), jnp.float32)
        for n in range(width // cols):
            part = pl.ds(n * cols, cols)
            term = jnp.dot(grads, weight(l, n, cols), preferred_element_type=jnp.float32)
            saved = jnp.concatenate(
                [
                    saved_ref[l, where, parity, :, part].reshape(span // 2, cols)
                    for where in (near, away)
                ],
                axis=0,
            )
            product = term * saved.astype(jnp.float32)
            for k in range(cols // LANES):
                score = score + product[:, k * LANES : (k + 1) * LANES]
            out = (term * scale).astype(jnp.bfloat16)
            keep_ref[l, :, part] = out[: span // 2]
            send_ref[l, :, part] = out[span // 2 :]
        score = jnp.sum(score, axis=1, keepdims=True)
        spread = jnp.where(lax.rem(part_row, capacity) + l * capacity == part_lane, score, 0.0)
        sent = sent + jnp.sum(spread.reshape(count, capacity, LANES), axis=1)
    turned = jnp.concatenate([sent[count // 2 :], sent[: count // 2]], axis=0)
    return jnp.where(side == 0, sent, turned)


def first_kernel(local, groups, capacity, *refs):
    count = groups // 2
    blocks, sources = refs[:count], refs[count : count + 3]
    w_ref, h_ref, r_ref, keep_ref, send_ref, score_ref, w_sems, sems = refs[count + 3 :]
    cols = w_ref.shape[2] // w_sems.shape[1]

    def fetch(l, n):
        part = pl.ds(n * cols, cols)
        return pltpu.make_async_copy(
            sources[0].at[l, :, part], w_ref.at[l, :, part], w_sems.at[l, n]
        )

    others = [
        pltpu.make_async_copy(sources[1], h_ref, sems.at[0]),
        pltpu.make_async_copy(sources[2], r_ref, sems.at[1]),
    ]
    fetch(0, 0).start()
    others[0].start()
    for i in range(1, local * w_sems.shape[1]):
        fetch(i // w_sems.shape[1], i % w_sems.shape[1]).start()
    others[1].start()
    waited = set()

    def weight(l, n, size):
        piece = n * size // cols
        if (l, piece) not in waited:
            fetch(l, piece).wait()
            if not waited:
                others[0].wait()
            waited.add((l, piece))
        return w_ref[l, :, pl.ds(n * size, size)]

    score_ref[...] = half_of(
        lax.rem(lax.axis_index("grp"), 2),
        local,
        groups,
        capacity,
        blocks,
        h_ref,
        weight,
        (keep_ref, send_ref),
    )
    others[1].wait()


def second_kernel(local, groups, capacity, *refs):
    count = groups // 2
    blocks = refs[:count]
    w_ref, h_ref, other_ref, keep_ref, send_ref, score_ref = refs[count:]
    parity = 1 - lax.rem(lax.axis_index("grp"), 2)

    def weight(l, n, size):
        return w_ref[l, :, pl.ds(n * size, size)]

    mine = half_of(
        parity, local, groups, capacity, blocks, h_ref, weight, (keep_ref, send_ref)
    )
    other = other_ref[...]
    for x in range(2):
        value = jnp.where(parity == x, mine, other)
        score_ref[:, x] = jnp.broadcast_to(
            value[:, None, :], (count,) + score_ref.shape[2:]
        )


def weight_kernel(local, groups, capacity, parts, *refs):
    blocks = refs[:groups]
    h_ref, out_hbm, turned_buf, scaled_buf, out_buf, sems = refs[groups:]
    features = turned_buf.shape[0]
    tile = features // parts
    block_rows = blocks[0].shape[0]
    span = groups * capacity
    tokens = groups * block_rows
    own = lax.axis_index("grp")
    rows = jnp.concatenate([b[:, :features] for b in blocks], axis=0)
    turned_buf[...] = rows.T
    aux = jnp.concatenate([b[:, features:] for b in blocks], axis=0).astype(jnp.float32)
    at = iota(aux.shape, 1)
    source = (iota((tokens, 1), 0) // block_rows) ^ own
    copies = []
    for l in range(local):
        lane = l * groups + own
        prob = jnp.sum(jnp.where(at == lane, aux, 0.0), axis=1, keepdims=True)
        rank = jnp.sum(jnp.where(at == local * groups + lane, aux, 0.0), axis=1, keepdims=True)
        place = jnp.where(rank > 0, source * capacity + rank.astype(jnp.int32) - 1, -1)
        pick = jnp.where(place == iota((tokens, span), 1), prob, 0.0).astype(jnp.bfloat16)
        scaled_buf[...] = jnp.dot(
            turned_buf[...], pick, preferred_element_type=jnp.float32
        ).astype(jnp.bfloat16)
        for d in range(parts):
            part = pl.ds(d * tile, tile)
            out_buf[l, part] = jnp.dot(
                scaled_buf[part], h_ref[l], preferred_element_type=jnp.float32
            ).astype(jnp.bfloat16)
            copy = pltpu.make_async_copy(
                out_buf.at[l, part], out_hbm.at[l, part], sems.at[l * parts + d]
            )
            copy.start()
            copies.append(copy)
    for copy in copies:
        copy.wait()


def pair_kernel(mine_a, got_a, mine_b, got_b, keep_ref, send_ref):
    bit = lax.axis_index("ep") // 2
    parity = lax.rem(lax.axis_index("grp"), 2)
    shape = keep_ref.shape[:1] + keep_ref.shape[2:]
    for at, mine, got in ((parity, mine_a, got_a), (1 - parity, mine_b, got_b)):
        kept_sum = mine[bit].astype(jnp.float32) + got[bit].astype(jnp.float32)
        sent_sum = mine[1 - bit].astype(jnp.float32) + got[1 - bit].astype(jnp.float32)
        keep_ref[:, at] = kept_sum.reshape(shape)
        send_ref[:, at] = sent_sum.astype(jnp.bfloat16).reshape(shape)


def router_kernel(local, capacity, score_ref, meta_ref, w_ref, out_ref):
    groups, tokens = meta_ref.shape[2], out_ref.shape[0]
    found = jnp.sum(score_ref[...], axis=1)
    scores = []
    for l in range(local):
        rank = meta_ref[l, 2].astype(jnp.int32)
        at = jnp.maximum(rank + (l * capacity - 1), 0)
        value = jnp.take_along_axis(found, at, axis=1, mode="promise_in_bounds")
        scores.append(jnp.where(rank > 0, value, 0.0))
    mean = sum(
        jnp.sum(meta_ref[l, 1] * scores[l], axis=0, keepdims=True) for l in range(local)
    ) * (1.0 / route_scale)
    grads = jnp.concatenate(
        [
            meta_ref[l, 1] * (1.0 - meta_ref[l, 0]) * (scores[l] - mean)
            for l in range(local)
        ],
        axis=0,
    ).astype(jnp.bfloat16)
    count = local * groups
    row = iota((count, count), 0)
    expert = lax.rem(row, groups) * local + row // groups
    order = (expert == iota((count, count), 1)).astype(jnp.bfloat16)
    turned = contract_rows(grads, order)[:tokens].astype(jnp.bfloat16)
    out_ref[...] = jnp.dot(turned, w_ref[...], preferred_element_type=jnp.float32).astype(
        jnp.bfloat16
    )


def cost(flops, nbytes):
    return pl.CostEstimate(flops=flops, bytes_accessed=nbytes, transcendentals=0)


def struct(shape, dtype):
    return jax.ShapeDtypeStruct(shape, dtype)


def held(x):
    return pltpu.with_memory_space_constraint(x, pltpu.VMEM)


def away_from_vmem(x):
    return pltpu.with_memory_space_constraint(x, pltpu.HBM)


def kept(shape, dtype):
    return pltpu.VMEM(shape, dtype)


def token_plan(out_grad, expert_ids, router_logits, router_weight, expert_weight, hidden_saved):
    group_rows, features = out_grad.shape
    groups, ep_count = lax.axis_size("grp"), lax.axis_size("ep")
    local, _, width = expert_weight.shape
    slot_count = hidden_saved.shape[1]
    capacity = slot_count // (local * groups)
    span = groups * capacity
    tokens = groups * group_rows
    bf16, f32 = jnp.bfloat16, jnp.float32
    vmem = pl.BlockSpec(memory_space=pltpu.VMEM)
    hbm = pl.BlockSpec(memory_space=pltpu.HBM)

    def limit(mib):
        return pltpu.CompilerParams(vmem_limit_bytes=mib * 2**20)

    packed, meta = pl.pallas_call(
        functools.partial(pack_kernel, local),
        out_shape=(
            pltpu.VMEM((group_rows, features + LANES), bf16),
            pltpu.VMEM((local, 3, groups, LANES), f32),
        ),
        in_specs=[hbm] * 3,
        out_specs=(vmem, vmem),
        scratch_shapes=[
            pltpu.VMEM(expert_ids.shape[::-1], jnp.int32),
            pltpu.VMEM(router_logits.shape[::-1], f32),
            pltpu.SemaphoreType.DMA((3,)),
        ],
        compiler_params=limit(2),
        name="pack",
    )(away_from_vmem(expert_ids.T), away_from_vmem(router_logits.T), away_from_vmem(out_grad))
    blocks = [held(b) for b in gather_blocks(packed)]

    saved_shape = (local, groups // 2, 2, capacity, width)
    sums = [kept((local, span // 4, width), bf16)] * 2
    work = slot_count * features * width
    weights, saved, projection, keep_a, send_a, score_a = pl.pallas_call(
        functools.partial(first_kernel, local, groups, capacity),
        out_shape=(
            kept(expert_weight.shape, bf16),
            kept(saved_shape, bf16),
            kept(router_weight.shape, bf16),
            *sums,
            kept((groups // 2, LANES), f32),
        ),
        in_specs=[vmem] * (groups // 2) + [hbm] * 3,
        out_specs=(vmem,) * 6,
        scratch_shapes=[pltpu.SemaphoreType.DMA((local, 1)), pltpu.SemaphoreType.DMA((2,))],
        compiler_params=limit(8),
        cost_estimate=cost(work, 8 * 2**20),
        name="first",
    )(
        *blocks[0::2],
        away_from_vmem(expert_weight),
        away_from_vmem(hidden_saved.reshape(saved_shape)),
        away_from_vmem(router_weight),
    )
    core_pairs = [(i, i ^ 1) for i in range(ep_count)]
    chip_pairs = [(i, i ^ 2) for i in range(ep_count)]
    got_a = lax.ppermute(send_a, "ep", core_pairs)

    keep_b, send_b, score = pl.pallas_call(
        functools.partial(second_kernel, local, groups, capacity),
        out_shape=(*sums, kept((groups // 2, 2, ep_count, LANES), f32)),
        in_specs=[vmem] * (groups // 2 + 3),
        out_specs=(vmem,) * 3,
        compiler_params=limit(8),
        cost_estimate=cost(work, 4 * 2**20),
        name="second",
    )(*blocks[1::2], held(weights), held(saved), held(score_a))
    got_b = lax.ppermute(send_b, "ep", core_pairs)
    from_all = lax.all_to_all(
        score.reshape(groups * ep_count, 1, LANES), ("grp", "ep"), 0, 0, tiled=True
    )
    order = (groups // 4, 2, capacity, width)
    mine, away = pl.pallas_call(
        pair_kernel,
        out_shape=(kept(order, f32), kept(order, bf16)),
        in_specs=[vmem] * 4,
        out_specs=(vmem, vmem),
        compiler_params=limit(2),
        name="pair",
    )(held(keep_a), held(got_a), held(keep_b), held(got_b))
    last = lax.ppermute(away, "ep", chip_pairs)

    parts = 4
    weight_grad = pl.pallas_call(
        functools.partial(weight_kernel, local, groups, capacity, parts),
        out_shape=struct((local, features, width), bf16),
        in_specs=[vmem] * (groups + 1),
        out_specs=hbm,
        scratch_shapes=[
            pltpu.VMEM((features, tokens), bf16),
            pltpu.VMEM((features, span), bf16),
            pltpu.VMEM((local, features, width), bf16),
            pltpu.SemaphoreType.DMA((local * parts,)),
        ],
        compiler_params=limit(12),
        cost_estimate=cost(2 * slot_count * features * width, 6 * 2**20),
        name="weight",
    )(*blocks, held(saved.reshape(local, span, width)))

    hidden_grad = (mine + last.astype(f32)).astype(bf16).reshape(1, span // 2, width)

    input_grad = pl.pallas_call(
        functools.partial(router_kernel, local, capacity),
        out_shape=struct((group_rows, features), bf16),
        in_specs=[vmem] * 3,
        out_specs=vmem,
        compiler_params=limit(2),
        name="router",
    )(held(from_all.reshape(groups, ep_count, LANES)), held(meta), held(projection))
    return (weight_grad, hidden_grad, input_grad)


def body(out_grad, expert_ids, router_logits, router_weight, expert_weight, hidden_saved):
    groups, ep_count = lax.axis_size("grp"), lax.axis_size("ep")
    rows, experts = router_logits.shape
    slots = hidden_saved.shape[1]
    local = expert_weight.shape[0]
    fits = (
        rows * groups <= slots
        and groups % 8 == 0
        and groups & (groups - 1) == 0
        and (local, ep_count) == (2, 4)
        and rows % 16 == 0
        and slots // groups <= LANES
        and 2 * experts <= LANES
    )
    plan = token_plan if fits else slot_plan
    return plan(
        out_grad, expert_ids, router_logits, router_weight, expert_weight, hidden_saved
    )


def solution(mesh):
    in_specs = (
        P("grp", "ep"),
        P("grp", None),
        P("grp", None),
        P(None, "ep"),
        P("grp", "ep", None),
        P("grp", None, None),
    )
    out_specs = (P("grp", "ep", None), P("grp", "ep", None), P("grp", "ep"))
    return jax.shard_map(body, mesh=mesh, in_specs=in_specs, out_specs=out_specs, check_vma=False)
```

```python
import functools

import jax
import jax.numpy as jnp
from jax import lax
from jax.experimental import pallas as pl
from jax.experimental.pallas import tpu as pltpu
from jax.sharding import PartitionSpec as P


route_scale = 2.5
LANES = 128


def slot_plan(out_grad, expert_ids, router_logits, router_weight, expert_weight, hidden_saved):
    group_rows, features = out_grad.shape
    top_count = expert_ids.shape[1]
    experts = router_logits.shape[1]
    group_count = lax.axis_size("grp")
    local_experts = expert_weight.shape[0]
    hidden_width = expert_weight.shape[2]
    slot_count = hidden_saved.shape[1]
    capacity = slot_count // (local_experts * group_count)
    expert_span = group_count * capacity
    pair_count = group_rows * top_count
    sig_values = jax.nn.sigmoid(router_logits)
    picked = expert_ids[:, :, None] == jnp.arange(experts, dtype=jnp.int32)[None, None, :]
    chosen = jnp.sum(jnp.where(picked, sig_values[:, None, :], 0.0), axis=2)
    route_probs = route_scale * chosen / jnp.sum(chosen, axis=1, keepdims=True)
    flat_ids = expert_ids.reshape(pair_count)
    onehot = picked.reshape(pair_count, experts).astype(jnp.int32)
    pair_ranks = jnp.sum((jnp.cumsum(onehot, axis=0) - 1) * onehot, axis=1)
    slot_place = (
        flat_ids % local_experts * group_count + flat_ids // local_experts
    ) * capacity + pair_ranks
    slot_match = slot_place[None, :] == jnp.arange(slot_count, dtype=jnp.int32)[:, None]
    token_pick = jnp.sum(
        slot_match.reshape(slot_count, group_rows, top_count).astype(jnp.float32), axis=2
    ).astype(jnp.bfloat16)
    send_rows = jnp.dot(token_pick, out_grad, preferred_element_type=jnp.float32).astype(
        jnp.bfloat16
    )
    send_prob = jnp.sum(
        jnp.where(slot_match, route_probs.reshape(1, pair_count), 0.0), axis=1
    ).astype(jnp.bfloat16)
    swap = dict(split_axis=1, concat_axis=1, tiled=True)
    shape = (local_experts, group_count, capacity)
    got_rows = lax.all_to_all(send_rows.reshape(shape + (features,)), "grp", **swap)
    got_prob = lax.all_to_all(send_prob.reshape(shape), "grp", **swap)
    slot_grads = got_rows.reshape(local_experts, expert_span, features)
    prob_rows = got_prob.reshape(local_experts, expert_span).astype(jnp.float32)
    saved_rows = hidden_saved.reshape(local_experts, expert_span, hidden_width)
    scaled_rows = (prob_rows[:, :, None] * slot_grads.astype(jnp.float32)).astype(jnp.bfloat16)
    weight_grad = jnp.einsum(
        "lmd,lmf->ldf", scaled_rows, saved_rows, preferred_element_type=jnp.float32
    ).astype(jnp.bfloat16)
    owner_index = lax.axis_index("ep")
    share_rows = slot_count // lax.axis_size("ep")
    flat_prob = prob_rows.reshape(slot_count)
    flat_saved = hidden_saved.reshape(slot_count, hidden_width)
    partial_term = jnp.einsum(
        "lmd,ldf->lmf", slot_grads, expert_weight, preferred_element_type=jnp.float32
    ).reshape(slot_count, hidden_width)
    rounded_term = lax.optimization_barrier(partial_term.astype(jnp.bfloat16)).astype(jnp.float32)
    partial_score = jnp.sum(flat_saved.astype(jnp.float32) * rounded_term, axis=1)
    moved_scores = lax.all_to_all(partial_score.reshape(shape), "grp", **swap)
    returned = lax.psum(moved_scores, "ep")
    summed = lax.psum_scatter(
        partial_term.astype(jnp.bfloat16), "ep", scatter_dimension=0, tiled=True
    ).astype(jnp.float32)
    own_prob = lax.dynamic_slice_in_dim(flat_prob, owner_index * share_rows, share_rows, 0)
    hidden_grad = (own_prob[:, None] * summed).astype(jnp.bfloat16)[None]
    pair_score = jnp.sum(
        jnp.where(slot_match, returned.reshape(slot_count, 1), 0.0), axis=0
    ).reshape(group_rows, top_count)
    weighted_mean = jnp.sum(route_probs * pair_score, axis=1, keepdims=True) / route_scale
    logit_terms = route_probs * (1.0 - chosen) * (pair_score - weighted_mean)
    router_grad = jnp.sum(jnp.where(picked, logit_terms[:, :, None], 0.0), axis=1).astype(
        jnp.bfloat16
    )
    input_grad = jnp.dot(router_grad, router_weight, preferred_element_type=jnp.float32).astype(
        jnp.bfloat16
    )
    return (weight_grad, hidden_grad, input_grad)


def exchange(x, distance):
    count = lax.axis_size("grp")
    return lax.ppermute(x, "grp", [(i, i ^ distance) for i in range(count)])


def swap_order(count):
    top, rest = count - 2, list(range(2, count - 2, 2))
    return [top, 1] + rest + [top ^ 1, 3] + [d ^ 1 for d in rest if d != 2]


def gather_blocks(x):
    count = lax.axis_size("grp")
    blocks = {0: x}
    for distance in swap_order(count):
        if distance == 3:
            source, step = 1, 2
        else:
            source, step = (distance ^ 1, 1) if distance & 1 else (0, distance)
        blocks[distance] = exchange(blocks[source], step)
    return [blocks[d] for d in range(count)]


def iota(shape, dim):
    return lax.broadcasted_iota(jnp.int32, shape, dim)


def contract_rows(a, b):
    return lax.dot_general(a, b, (((0,), (0,)), ((), ())), preferred_element_type=jnp.float32)


def pack_kernel(local, ids_hbm, logits_hbm, rows_hbm, packed_ref, meta_ref, ids_ref, logits_ref, sems):
    top_count, tokens = ids_ref.shape
    groups = logits_ref.shape[0] // local
    features = rows_hbm.shape[1]
    copies = [
        pltpu.make_async_copy(ids_hbm, ids_ref, sems.at[0]),
        pltpu.make_async_copy(logits_hbm, logits_ref, sems.at[1]),
        pltpu.make_async_copy(rows_hbm, packed_ref.at[:, pl.ds(0, features)], sems.at[2]),
    ]
    for c in copies:
        c.start()
    copies[0].wait()
    copies[1].wait()
    ids = ids_ref[...]
    upto = (iota((tokens, tokens), 0) <= iota((tokens, tokens), 1)).astype(jnp.bfloat16)
    sig, chosen, ranks = [], [], []
    for l in range(local):
        expert = iota((groups, tokens), 0) * local + l
        hit = jnp.zeros((groups, tokens), jnp.float32)
        for i in range(top_count):
            hit = hit + (ids[i : i + 1, :] == expert).astype(jnp.float32)
        value = jax.nn.sigmoid(logits_ref[pl.ds(l, groups, stride=local), :])
        sig.append(value)
        chosen.append(hit * value)
        count = jnp.dot(hit.astype(jnp.bfloat16), upto, preferred_element_type=jnp.float32)
        ranks.append(hit * count)
    total = sum(jnp.sum(c, axis=0, keepdims=True) for c in chosen)
    probs = [route_scale * c / total for c in chosen]
    stack = jnp.concatenate(probs + ranks, axis=0).astype(jnp.bfloat16)
    lanes = packed_ref.shape[1] - features
    spread = (iota((stack.shape[0], lanes), 0) == iota((stack.shape[0], lanes), 1)).astype(
        jnp.bfloat16
    )
    packed_ref[:, features:] = contract_rows(stack, spread).astype(jnp.bfloat16)
    for l in range(local):
        for k, value in enumerate((sig[l], probs[l], ranks[l])):
            meta_ref[l, k] = jnp.zeros(meta_ref.shape[2:], jnp.float32)
            meta_ref[l, k, :, :tokens] = value
    copies[2].wait()


def half_of(parity, local, groups, capacity, blocks, saved_ref, weight, outs):
    keep_ref, send_ref = outs
    block_rows, features = blocks[0].shape[0], blocks[0].shape[1] - LANES
    width = keep_ref.shape[2]
    count = groups // 2
    span, tokens = count * capacity, count * block_rows
    cols = 256 if width % 256 == 0 else LANES
    own, side = lax.axis_index("grp"), lax.rem(lax.axis_index("ep"), 2)
    rows = jnp.concatenate([b[:, :features] for b in blocks], axis=0)
    aux = jnp.concatenate([b[:, features:] for b in blocks], axis=0).astype(jnp.float32).T
    source = (iota((1, tokens), 1) // block_rows) ^ (own // 2)
    slot = iota((span, tokens), 0) + side * (span // 2)
    slot = jnp.where(slot >= span, slot - span, slot)
    near = pl.ds(side * (count // 2), count // 2)
    away = pl.ds((1 - side) * (count // 2), count // 2)
    part_row, part_lane = iota((span, LANES), 0), iota((span, LANES), 1)
    sent = jnp.zeros((count, LANES), jnp.float32)
    for l in range(local):
        lane = l * groups + own
        row = iota(aux.shape, 0)
        prob = jnp.sum(jnp.where(row == lane, aux, 0.0), axis=0, keepdims=True)
        rank = jnp.sum(jnp.where(row == local * groups + lane, aux, 0.0), axis=0, keepdims=True)
        place = jnp.where(rank > 0, source * capacity + rank.astype(jnp.int32) - 1, -1)
        pick = slot == place
        scale = jnp.sum(jnp.where(pick, prob, 0.0), axis=1, keepdims=True)
        grads = jnp.dot(
            pick.astype(jnp.float32).astype(jnp.bfloat16), rows, preferred_element_type=jnp.float32
        ).astype(jnp.bfloat16)
        score = jnp.zeros((span, LANES), jnp.float32)
        for n in range(width // cols):
            part = pl.ds(n * cols, cols)
            term = jnp.dot(grads, weight(l, n, cols), preferred_element_type=jnp.float32)
            saved = jnp.concatenate(
                [
                    saved_ref[l, where, parity, :, part].reshape(span // 2, cols)
                    for where in (near, away)
                ],
                axis=0,
            )
            product = term * saved.astype(jnp.float32)
            for k in range(cols // LANES):
                score = score + product[:, k * LANES : (k + 1) * LANES]
            out = (term * scale).astype(jnp.bfloat16)
            keep_ref[l, :, part] = out[: span // 2]
            send_ref[l, :, part] = out[span // 2 :]
        score = jnp.sum(score, axis=1, keepdims=True)
        spread = jnp.where(lax.rem(part_row, capacity) + l * capacity == part_lane, score, 0.0)
        sent = sent + jnp.sum(spread.reshape(count, capacity, LANES), axis=1)
    turned = jnp.concatenate([sent[count // 2 :], sent[: count // 2]], axis=0)
    return jnp.where(side == 0, sent, turned)


def first_kernel(local, groups, capacity, *refs):
    count = groups // 2
    blocks, sources = refs[:count], refs[count : count + 3]
    w_ref, h_ref, r_ref, keep_ref, send_ref, score_ref, w_sems, sems = refs[count + 3 :]
    cols = w_ref.shape[2] // w_sems.shape[1]

    def fetch(l, n):
        part = pl.ds(n * cols, cols)
        return pltpu.make_async_copy(
            sources[0].at[l, :, part], w_ref.at[l, :, part], w_sems.at[l, n]
        )

    others = [
        pltpu.make_async_copy(sources[1], h_ref, sems.at[0]),
        pltpu.make_async_copy(sources[2], r_ref, sems.at[1]),
    ]
    fetch(0, 0).start()
    others[0].start()
    for i in range(1, local * w_sems.shape[1]):
        fetch(i // w_sems.shape[1], i % w_sems.shape[1]).start()
    others[1].start()
    waited = set()

    def weight(l, n, size):
        piece = n * size // cols
        if (l, piece) not in waited:
            fetch(l, piece).wait()
            if not waited:
                others[0].wait()
            waited.add((l, piece))
        return w_ref[l, :, pl.ds(n * size, size)]

    score_ref[...] = half_of(
        lax.rem(lax.axis_index("grp"), 2),
        local,
        groups,
        capacity,
        blocks,
        h_ref,
        weight,
        (keep_ref, send_ref),
    )
    others[1].wait()


def second_kernel(local, groups, capacity, *refs):
    count = groups // 2
    blocks = refs[:count]
    w_ref, h_ref, other_ref, keep_ref, send_ref, score_ref = refs[count:]
    parity = 1 - lax.rem(lax.axis_index("grp"), 2)

    def weight(l, n, size):
        return w_ref[l, :, pl.ds(n * size, size)]

    mine = half_of(
        parity, local, groups, capacity, blocks, h_ref, weight, (keep_ref, send_ref)
    )
    other = other_ref[...]
    for x in range(2):
        value = jnp.where(parity == x, mine, other)
        score_ref[:, x] = jnp.broadcast_to(
            value[:, None, :], (count,) + score_ref.shape[2:]
        )


def weight_kernel(local, groups, capacity, parts, *refs):
    blocks = refs[:groups]
    h_ref, out_hbm, turned_buf, scaled_buf, out_buf, sems = refs[groups:]
    features = turned_buf.shape[0]
    tile = features // parts
    block_rows = blocks[0].shape[0]
    span = groups * capacity
    tokens = groups * block_rows
    own = lax.axis_index("grp")
    rows = jnp.concatenate([b[:, :features] for b in blocks], axis=0)
    turned_buf[...] = rows.T
    aux = jnp.concatenate([b[:, features:] for b in blocks], axis=0).astype(jnp.float32)
    at = iota(aux.shape, 1)
    source = (iota((tokens, 1), 0) // block_rows) ^ own
    copies = []
    for l in range(local):
        lane = l * groups + own
        prob = jnp.sum(jnp.where(at == lane, aux, 0.0), axis=1, keepdims=True)
        rank = jnp.sum(jnp.where(at == local * groups + lane, aux, 0.0), axis=1, keepdims=True)
        place = jnp.where(rank > 0, source * capacity + rank.astype(jnp.int32) - 1, -1)
        pick = jnp.where(place == iota((tokens, span), 1), prob, 0.0).astype(jnp.bfloat16)
        scaled_buf[...] = jnp.dot(
            turned_buf[...], pick, preferred_element_type=jnp.float32
        ).astype(jnp.bfloat16)
        for d in range(parts):
            part = pl.ds(d * tile, tile)
            out_buf[l, part] = jnp.dot(
                scaled_buf[part], h_ref[l], preferred_element_type=jnp.float32
            ).astype(jnp.bfloat16)
            copy = pltpu.make_async_copy(
                out_buf.at[l, part], out_hbm.at[l, part], sems.at[l * parts + d]
            )
            copy.start()
            copies.append(copy)
    for copy in copies:
        copy.wait()


def pair_kernel(mine_ref, got_ref, keep_ref, send_ref):
    bit = lax.axis_index("ep") // 2
    keep_ref[...] = mine_ref[bit].astype(jnp.float32) + got_ref[bit].astype(jnp.float32)
    send_ref[...] = (
        mine_ref[1 - bit].astype(jnp.float32) + got_ref[1 - bit].astype(jnp.float32)
    ).astype(jnp.bfloat16)


def last_kernel(mine_a, got_a, mine_b, got_b, out_ref):
    parity = lax.rem(lax.axis_index("grp"), 2)
    shape = out_ref.shape[:1] + out_ref.shape[2:]
    for at, mine, got in ((parity, mine_a, got_a), (1 - parity, mine_b, got_b)):
        total = mine[...] + got[...].astype(jnp.float32)
        out_ref[:, at] = total.astype(jnp.bfloat16).reshape(shape)


def router_kernel(local, capacity, score_ref, meta_ref, w_ref, out_ref):
    groups, tokens = meta_ref.shape[2], out_ref.shape[0]
    found = jnp.sum(score_ref[...], axis=1)
    scores = []
    for l in range(local):
        rank = meta_ref[l, 2].astype(jnp.int32)
        at = jnp.maximum(rank + (l * capacity - 1), 0)
        value = jnp.take_along_axis(found, at, axis=1, mode="promise_in_bounds")
        scores.append(jnp.where(rank > 0, value, 0.0))
    mean = sum(
        jnp.sum(meta_ref[l, 1] * scores[l], axis=0, keepdims=True) for l in range(local)
    ) * (1.0 / route_scale)
    grads = jnp.concatenate(
        [
            meta_ref[l, 1] * (1.0 - meta_ref[l, 0]) * (scores[l] - mean)
            for l in range(local)
        ],
        axis=0,
    ).astype(jnp.bfloat16)
    count = local * groups
    row = iota((count, count), 0)
    expert = lax.rem(row, groups) * local + row // groups
    order = (expert == iota((count, count), 1)).astype(jnp.bfloat16)
    turned = contract_rows(grads, order)[:tokens].astype(jnp.bfloat16)
    out_ref[...] = jnp.dot(turned, w_ref[...], preferred_element_type=jnp.float32).astype(
        jnp.bfloat16
    )


def cost(flops, nbytes):
    return pl.CostEstimate(flops=flops, bytes_accessed=nbytes, transcendentals=0)


def struct(shape, dtype):
    return jax.ShapeDtypeStruct(shape, dtype)


def held(x):
    return pltpu.with_memory_space_constraint(x, pltpu.VMEM)


def away_from_vmem(x):
    return pltpu.with_memory_space_constraint(x, pltpu.HBM)


def kept(shape, dtype):
    return pltpu.VMEM(shape, dtype)


def token_plan(out_grad, expert_ids, router_logits, router_weight, expert_weight, hidden_saved):
    group_rows, features = out_grad.shape
    groups, ep_count = lax.axis_size("grp"), lax.axis_size("ep")
    local, _, width = expert_weight.shape
    slot_count = hidden_saved.shape[1]
    capacity = slot_count // (local * groups)
    span = groups * capacity
    tokens = groups * group_rows
    bf16, f32 = jnp.bfloat16, jnp.float32
    vmem = pl.BlockSpec(memory_space=pltpu.VMEM)
    hbm = pl.BlockSpec(memory_space=pltpu.HBM)

    def limit(mib):
        return pltpu.CompilerParams(vmem_limit_bytes=mib * 2**20)

    packed, meta = pl.pallas_call(
        functools.partial(pack_kernel, local),
        out_shape=(
            pltpu.VMEM((group_rows, features + LANES), bf16),
            pltpu.VMEM((local, 3, groups, LANES), f32),
        ),
        in_specs=[hbm] * 3,
        out_specs=(vmem, vmem),
        scratch_shapes=[
            pltpu.VMEM(expert_ids.shape[::-1], jnp.int32),
            pltpu.VMEM(router_logits.shape[::-1], f32),
            pltpu.SemaphoreType.DMA((3,)),
        ],
        compiler_params=limit(2),
        name="pack",
    )(away_from_vmem(expert_ids.T), away_from_vmem(router_logits.T), away_from_vmem(out_grad))
    blocks = [held(b) for b in gather_blocks(packed)]

    saved_shape = (local, groups // 2, 2, capacity, width)
    sums = [kept((local, span // 4, width), bf16)] * 2
    work = slot_count * features * width
    core_pairs = [(i, i ^ 1) for i in range(ep_count)]
    chip_pairs = [(i, i ^ 2) for i in range(ep_count)]

    def both_cores(keep, send):
        got = lax.ppermute(send, "ep", core_pairs)
        return pl.pallas_call(
            pair_kernel,
            out_shape=(kept((span // 4, width), f32), kept((span // 4, width), bf16)),
            in_specs=[vmem] * 2,
            out_specs=(vmem,) * 2,
            compiler_params=limit(2),
        )(held(keep), held(got))

    weights, saved, projection, keep_a, send_a, score_a = pl.pallas_call(
        functools.partial(first_kernel, local, groups, capacity),
        out_shape=(
            kept(expert_weight.shape, bf16),
            kept(saved_shape, bf16),
            kept(router_weight.shape, bf16),
            *sums,
            kept((groups // 2, LANES), f32),
        ),
        in_specs=[vmem] * (groups // 2) + [hbm] * 3,
        out_specs=(vmem,) * 6,
        scratch_shapes=[pltpu.SemaphoreType.DMA((local, 1)), pltpu.SemaphoreType.DMA((2,))],
        compiler_params=limit(8),
        cost_estimate=cost(work, 8 * 2**20),
        name="first",
    )(
        *blocks[0::2],
        away_from_vmem(expert_weight),
        away_from_vmem(hidden_saved.reshape(saved_shape)),
        away_from_vmem(router_weight),
    )
    mine_a, away_a = both_cores(keep_a, send_a)
    last_a = lax.ppermute(away_a, "ep", chip_pairs)

    keep_b, send_b, score = pl.pallas_call(
        functools.partial(second_kernel, local, groups, capacity),
        out_shape=(*sums, kept((groups // 2, 2, ep_count, LANES), f32)),
        in_specs=[vmem] * (groups // 2 + 3),
        out_specs=(vmem,) * 3,
        compiler_params=limit(8),
        cost_estimate=cost(work, 4 * 2**20),
        name="second",
    )(*blocks[1::2], held(weights), held(saved), held(score_a))
    mine_b, away_b = both_cores(keep_b, send_b)
    from_all = lax.all_to_all(
        score.reshape(groups * ep_count, 1, LANES), ("grp", "ep"), 0, 0, tiled=True
    )
    last_b = lax.ppermute(away_b, "ep", chip_pairs)

    parts = 4
    weight_grad = pl.pallas_call(
        functools.partial(weight_kernel, local, groups, capacity, parts),
        out_shape=struct((local, features, width), bf16),
        in_specs=[vmem] * (groups + 1),
        out_specs=hbm,
        scratch_shapes=[
            pltpu.VMEM((features, tokens), bf16),
            pltpu.VMEM((features, span), bf16),
            pltpu.VMEM((local, features, width), bf16),
            pltpu.SemaphoreType.DMA((local * parts,)),
        ],
        compiler_params=limit(12),
        cost_estimate=cost(2 * slot_count * features * width, 6 * 2**20),
        name="weight",
    )(*blocks, held(saved.reshape(local, span, width)))

    hidden_grad = pl.pallas_call(
        last_kernel,
        out_shape=struct((groups // 4, 2, capacity, width), bf16),
        in_specs=[vmem] * 4,
        out_specs=vmem,
        compiler_params=limit(2),
        name="last",
    )(held(mine_a), held(last_a), held(mine_b), held(last_b)).reshape(1, span // 2, width)

    input_grad = pl.pallas_call(
        functools.partial(router_kernel, local, capacity),
        out_shape=struct((group_rows, features), bf16),
        in_specs=[vmem] * 3,
        out_specs=vmem,
        compiler_params=limit(2),
        name="router",
    )(held(from_all.reshape(groups, ep_count, LANES)), held(meta), held(projection))
    return (weight_grad, hidden_grad, input_grad)


def body(out_grad, expert_ids, router_logits, router_weight, expert_weight, hidden_saved):
    groups, ep_count = lax.axis_size("grp"), lax.axis_size("ep")
    rows, experts = router_logits.shape
    slots = hidden_saved.shape[1]
    local = expert_weight.shape[0]
    fits = (
        rows * groups <= slots
        and groups % 8 == 0
        and groups & (groups - 1) == 0
        and (local, ep_count) == (2, 4)
        and rows % 16 == 0
        and slots // groups <= LANES
        and 2 * experts <= LANES
    )
    plan = token_plan if fits else slot_plan
    return plan(
        out_grad, expert_ids, router_logits, router_weight, expert_weight, hidden_saved
    )


def solution(mesh):
    in_specs = (
        P("grp", "ep"),
        P("grp", None),
        P("grp", None),
        P(None, "ep"),
        P("grp", "ep", None),
        P("grp", None, None),
    )
    out_specs = (P("grp", "ep", None), P("grp", "ep", None), P("grp", "ep"))
    return jax.shard_map(body, mesh=mesh, in_specs=in_specs, out_specs=out_specs, check_vma=False)
```

```python
import functools

import jax
import jax.numpy as jnp
from jax import lax
from jax.experimental import pallas as pl
from jax.experimental.pallas import tpu as pltpu
from jax.sharding import PartitionSpec as P


route_scale = 2.5
LANES = 128


def slot_plan(out_grad, expert_ids, router_logits, router_weight, expert_weight, hidden_saved):
    group_rows, features = out_grad.shape
    top_count = expert_ids.shape[1]
    experts = router_logits.shape[1]
    group_count = lax.axis_size("grp")
    local_experts = expert_weight.shape[0]
    hidden_width = expert_weight.shape[2]
    slot_count = hidden_saved.shape[1]
    capacity = slot_count // (local_experts * group_count)
    expert_span = group_count * capacity
    pair_count = group_rows * top_count
    sig_values = jax.nn.sigmoid(router_logits)
    picked = expert_ids[:, :, None] == jnp.arange(experts, dtype=jnp.int32)[None, None, :]
    chosen = jnp.sum(jnp.where(picked, sig_values[:, None, :], 0.0), axis=2)
    route_probs = route_scale * chosen / jnp.sum(chosen, axis=1, keepdims=True)
    flat_ids = expert_ids.reshape(pair_count)
    onehot = picked.reshape(pair_count, experts).astype(jnp.int32)
    pair_ranks = jnp.sum((jnp.cumsum(onehot, axis=0) - 1) * onehot, axis=1)
    slot_place = (
        flat_ids % local_experts * group_count + flat_ids // local_experts
    ) * capacity + pair_ranks
    slot_match = slot_place[None, :] == jnp.arange(slot_count, dtype=jnp.int32)[:, None]
    token_pick = jnp.sum(
        slot_match.reshape(slot_count, group_rows, top_count).astype(jnp.float32), axis=2
    ).astype(jnp.bfloat16)
    send_rows = jnp.dot(token_pick, out_grad, preferred_element_type=jnp.float32).astype(
        jnp.bfloat16
    )
    send_prob = jnp.sum(
        jnp.where(slot_match, route_probs.reshape(1, pair_count), 0.0), axis=1
    ).astype(jnp.bfloat16)
    swap = dict(split_axis=1, concat_axis=1, tiled=True)
    shape = (local_experts, group_count, capacity)
    got_rows = lax.all_to_all(send_rows.reshape(shape + (features,)), "grp", **swap)
    got_prob = lax.all_to_all(send_prob.reshape(shape), "grp", **swap)
    slot_grads = got_rows.reshape(local_experts, expert_span, features)
    prob_rows = got_prob.reshape(local_experts, expert_span).astype(jnp.float32)
    saved_rows = hidden_saved.reshape(local_experts, expert_span, hidden_width)
    scaled_rows = (prob_rows[:, :, None] * slot_grads.astype(jnp.float32)).astype(jnp.bfloat16)
    weight_grad = jnp.einsum(
        "lmd,lmf->ldf", scaled_rows, saved_rows, preferred_element_type=jnp.float32
    ).astype(jnp.bfloat16)
    owner_index = lax.axis_index("ep")
    share_rows = slot_count // lax.axis_size("ep")
    flat_prob = prob_rows.reshape(slot_count)
    flat_saved = hidden_saved.reshape(slot_count, hidden_width)
    partial_term = jnp.einsum(
        "lmd,ldf->lmf", slot_grads, expert_weight, preferred_element_type=jnp.float32
    ).reshape(slot_count, hidden_width)
    rounded_term = lax.optimization_barrier(partial_term.astype(jnp.bfloat16)).astype(jnp.float32)
    partial_score = jnp.sum(flat_saved.astype(jnp.float32) * rounded_term, axis=1)
    moved_scores = lax.all_to_all(partial_score.reshape(shape), "grp", **swap)
    returned = lax.psum(moved_scores, "ep")
    summed = lax.psum_scatter(
        partial_term.astype(jnp.bfloat16), "ep", scatter_dimension=0, tiled=True
    ).astype(jnp.float32)
    own_prob = lax.dynamic_slice_in_dim(flat_prob, owner_index * share_rows, share_rows, 0)
    hidden_grad = (own_prob[:, None] * summed).astype(jnp.bfloat16)[None]
    pair_score = jnp.sum(
        jnp.where(slot_match, returned.reshape(slot_count, 1), 0.0), axis=0
    ).reshape(group_rows, top_count)
    weighted_mean = jnp.sum(route_probs * pair_score, axis=1, keepdims=True) / route_scale
    logit_terms = route_probs * (1.0 - chosen) * (pair_score - weighted_mean)
    router_grad = jnp.sum(jnp.where(picked, logit_terms[:, :, None], 0.0), axis=1).astype(
        jnp.bfloat16
    )
    input_grad = jnp.dot(router_grad, router_weight, preferred_element_type=jnp.float32).astype(
        jnp.bfloat16
    )
    return (weight_grad, hidden_grad, input_grad)


def exchange(x, distance):
    count = lax.axis_size("grp")
    return lax.ppermute(x, "grp", [(i, i ^ distance) for i in range(count)])


def swap_order(count):
    top, rest = count - 2, list(range(2, count - 2, 2))
    return [top, 1] + rest + [3, top ^ 1] + [d ^ 1 for d in rest if d != 2]


def gather_blocks(x):
    count = lax.axis_size("grp")
    blocks = {0: x}
    for distance in swap_order(count):
        if distance == 3:
            source, step = 1, 2
        else:
            source, step = (distance ^ 1, 1) if distance & 1 else (0, distance)
        blocks[distance] = exchange(blocks[source], step)
    return [blocks[d] for d in range(count)]


def iota(shape, dim):
    return lax.broadcasted_iota(jnp.int32, shape, dim)


def contract_rows(a, b):
    return lax.dot_general(a, b, (((0,), (0,)), ((), ())), preferred_element_type=jnp.float32)


def pack_kernel(local, ids_hbm, logits_hbm, rows_hbm, packed_ref, meta_ref, ids_ref, logits_ref, sems):
    top_count, tokens = ids_ref.shape
    groups = logits_ref.shape[0] // local
    features = rows_hbm.shape[1]
    copies = [
        pltpu.make_async_copy(ids_hbm, ids_ref, sems.at[0]),
        pltpu.make_async_copy(logits_hbm, logits_ref, sems.at[1]),
        pltpu.make_async_copy(rows_hbm, packed_ref.at[:, pl.ds(0, features)], sems.at[2]),
    ]
    for c in copies:
        c.start()
    copies[0].wait()
    copies[1].wait()
    ids = ids_ref[...]
    upto = (iota((tokens, tokens), 0) <= iota((tokens, tokens), 1)).astype(jnp.bfloat16)
    sig, chosen, ranks = [], [], []
    for l in range(local):
        expert = iota((groups, tokens), 0) * local + l
        hit = jnp.zeros((groups, tokens), jnp.float32)
        for i in range(top_count):
            hit = hit + (ids[i : i + 1, :] == expert).astype(jnp.float32)
        value = jax.nn.sigmoid(logits_ref[pl.ds(l, groups, stride=local), :])
        sig.append(value)
        chosen.append(hit * value)
        count = jnp.dot(hit.astype(jnp.bfloat16), upto, preferred_element_type=jnp.float32)
        ranks.append(hit * count)
    total = sum(jnp.sum(c, axis=0, keepdims=True) for c in chosen)
    probs = [route_scale * c / total for c in chosen]
    stack = jnp.concatenate(probs + ranks, axis=0).astype(jnp.bfloat16)
    lanes = packed_ref.shape[1] - features
    spread = (iota((stack.shape[0], lanes), 0) == iota((stack.shape[0], lanes), 1)).astype(
        jnp.bfloat16
    )
    packed_ref[:, features:] = contract_rows(stack, spread).astype(jnp.bfloat16)
    for l in range(local):
        for k, value in enumerate((sig[l], probs[l], ranks[l])):
            meta_ref[l, k] = jnp.zeros(meta_ref.shape[2:], jnp.float32)
            meta_ref[l, k, :, :tokens] = value
    copies[2].wait()


def half_of(parity, experts, groups, capacity, blocks, saved_ref, w_ref, store):
    local = len(experts)
    block_rows, features = blocks[0].shape[0], blocks[0].shape[1] - LANES
    width = w_ref.shape[2]
    count = groups // 2
    span, tokens = count * capacity, count * block_rows
    cols = 256 if width % 256 == 0 else LANES
    own, side = lax.axis_index("grp"), lax.rem(lax.axis_index("ep"), 2)
    rows = jnp.concatenate([b[:, :features] for b in blocks], axis=0)
    aux = jnp.concatenate([b[:, features:] for b in blocks], axis=0).astype(jnp.float32).T
    source = (iota((1, tokens), 1) // block_rows) ^ (own // 2)
    slot = iota((span, tokens), 0) + side * (span // 2)
    slot = jnp.where(slot >= span, slot - span, slot)
    near = pl.ds(side * (count // 2), count // 2)
    away = pl.ds((1 - side) * (count // 2), count // 2)
    part_row, part_lane = iota((span, LANES), 0), iota((span, LANES), 1)
    sent = jnp.zeros((count, LANES), jnp.float32)
    row = iota(aux.shape, 0)
    picks, scales = [], []
    for l in experts:
        lane = l * groups + own
        prob = jnp.sum(jnp.where(row == lane, aux, 0.0), axis=0, keepdims=True)
        rank = jnp.sum(jnp.where(row == local * groups + lane, aux, 0.0), axis=0, keepdims=True)
        place = jnp.where(rank > 0, source * capacity + rank.astype(jnp.int32) - 1, -1)
        pick = slot == place
        picks.append(pick.astype(jnp.float32).astype(jnp.bfloat16))
        scales.append(jnp.sum(jnp.where(pick, prob, 0.0), axis=1, keepdims=True))
    grads = jnp.dot(
        jnp.concatenate(picks, axis=0), rows, preferred_element_type=jnp.float32
    ).astype(jnp.bfloat16)
    for i, l in enumerate(experts):
        score = jnp.zeros((span, LANES), jnp.float32)
        for n in range(width // cols):
            part = pl.ds(n * cols, cols)
            term = jnp.dot(
                grads[i * span : (i + 1) * span],
                w_ref[l, :, part],
                preferred_element_type=jnp.float32,
            )
            saved = jnp.concatenate(
                [
                    saved_ref[l, where, parity, :, part].reshape(span // 2, cols)
                    for where in (near, away)
                ],
                axis=0,
            )
            product = term * saved.astype(jnp.float32)
            for k in range(cols // LANES):
                score = score + product[:, k * LANES : (k + 1) * LANES]
            store(i, part, (term * scales[i]).astype(jnp.bfloat16))
        score = jnp.sum(score, axis=1, keepdims=True)
        spread = jnp.where(lax.rem(part_row, capacity) + l * capacity == part_lane, score, 0.0)
        sent = sent + jnp.sum(spread.reshape(count, capacity, LANES), axis=1)
    turned = jnp.concatenate([sent[count // 2 :], sent[: count // 2]], axis=0)
    return jnp.where(side == 0, sent, turned)


def load_kernel(cue_ref, *refs):
    sources, targets, sems = refs[:3], refs[3:6], refs[6]
    copies = [
        pltpu.make_async_copy(source, target, sems.at[i])
        for i, (source, target) in enumerate(zip(sources, targets))
    ]
    for copy in copies:
        copy.start()
    for copy in copies:
        copy.wait()


def first_kernel(groups, capacity, *refs):
    count = groups // 2
    blocks = refs[:count]
    w_ref, h_ref, keep_ref, send_ref, score_ref = refs[count:]
    bit = lax.axis_index("ep") // 2

    def store(i, part, value):
        (send_ref, keep_ref)[i][:, part] = value

    score_ref[...] = half_of(
        lax.rem(lax.axis_index("grp"), 2),
        (1 - bit, bit),
        groups,
        capacity,
        blocks,
        h_ref,
        w_ref,
        store,
    )


def second_kernel(local, groups, capacity, *refs):
    count = groups // 2
    blocks = refs[:count]
    w_ref, h_ref, other_ref, keep_ref, send_ref, score_ref = refs[count:]
    parity = 1 - lax.rem(lax.axis_index("grp"), 2)
    rows = keep_ref.shape[1]

    def store(l, part, value):
        keep_ref[l, :, part] = value[:rows]
        send_ref[l, :, part] = value[rows:]

    mine = half_of(
        parity, tuple(range(local)), groups, capacity, blocks, h_ref, w_ref, store
    )
    other = other_ref[...]
    for x in range(2):
        value = jnp.where(parity == x, mine, other)
        score_ref[:, x] = jnp.broadcast_to(
            value[:, None, :], (count,) + score_ref.shape[2:]
        )


def weight_kernel(local, groups, capacity, parts, *refs):
    blocks = refs[:groups]
    h_ref, r_ref, out_hbm, sorted_ref, turned_buf, scaled_buf, out_buf, sems = refs[groups:]
    experts = r_ref.shape[0]
    at = iota((experts, experts), 0)
    order = lax.rem(at, groups) * local + at // groups == iota((experts, experts), 1)
    sorted_ref[...] = jnp.dot(
        order.astype(jnp.float32).astype(jnp.bfloat16), r_ref[...], preferred_element_type=jnp.float32
    ).astype(jnp.bfloat16)
    features = turned_buf.shape[0]
    tile = features // parts
    block_rows = blocks[0].shape[0]
    span = groups * capacity
    tokens = groups * block_rows
    own = lax.axis_index("grp")
    rows = jnp.concatenate([b[:, :features] for b in blocks], axis=0)
    turned_buf[...] = rows.T
    aux = jnp.concatenate([b[:, features:] for b in blocks], axis=0).astype(jnp.float32)
    at = iota(aux.shape, 1)
    source = (iota((tokens, 1), 0) // block_rows) ^ own
    copies = []
    for l in range(local):
        lane = l * groups + own
        prob = jnp.sum(jnp.where(at == lane, aux, 0.0), axis=1, keepdims=True)
        rank = jnp.sum(jnp.where(at == local * groups + lane, aux, 0.0), axis=1, keepdims=True)
        place = jnp.where(rank > 0, source * capacity + rank.astype(jnp.int32) - 1, -1)
        pick = jnp.where(place == iota((tokens, span), 1), prob, 0.0).astype(jnp.bfloat16)
        scaled_buf[...] = jnp.dot(
            turned_buf[...], pick, preferred_element_type=jnp.float32
        ).astype(jnp.bfloat16)
        for d in range(parts):
            part = pl.ds(d * tile, tile)
            out_buf[l, part] = jnp.dot(
                scaled_buf[part], h_ref[l], preferred_element_type=jnp.float32
            ).astype(jnp.bfloat16)
            copy = pltpu.make_async_copy(
                out_buf.at[l, part], out_hbm.at[l, part], sems.at[l * parts + d]
            )
            copy.start()
            copies.append(copy)
    for copy in copies:
        copy.wait()


def pair_kernel(mine_ref, got_ref, keep_ref, send_ref):
    bit = lax.axis_index("ep") // 2
    keep_ref[...] = mine_ref[bit].astype(jnp.float32) + got_ref[bit].astype(jnp.float32)
    send_ref[...] = (
        mine_ref[1 - bit].astype(jnp.float32) + got_ref[1 - bit].astype(jnp.float32)
    ).astype(jnp.bfloat16)


def split_kernel(mine_ref, got_ref, keep_ref, send_ref):
    rows = keep_ref.shape[0]
    total = mine_ref[...].astype(jnp.float32) + got_ref[...].astype(jnp.float32)
    keep_ref[...] = total[:rows]
    send_ref[...] = total[rows:].astype(jnp.bfloat16)


def last_kernel(mine_a, got_a, mine_b, got_b, out_ref):
    parity = lax.rem(lax.axis_index("grp"), 2)
    shape = out_ref.shape[:1] + out_ref.shape[2:]
    for at, mine, got in ((parity, mine_a, got_a), (1 - parity, mine_b, got_b)):
        total = mine[...] + got[...].astype(jnp.float32)
        out_ref[:, at] = total.astype(jnp.bfloat16).reshape(shape)


def router_kernel(local, capacity, score_ref, meta_ref, w_ref, out_ref):
    tokens = out_ref.shape[0]
    found = jnp.sum(score_ref[...], axis=1)
    scores = []
    for l in range(local):
        rank = meta_ref[l, 2].astype(jnp.int32)
        at = jnp.maximum(rank + (l * capacity - 1), 0)
        value = jnp.take_along_axis(found, at, axis=1, mode="promise_in_bounds")
        scores.append(jnp.where(rank > 0, value, 0.0))
    mean = sum(
        jnp.sum(meta_ref[l, 1] * scores[l], axis=0, keepdims=True) for l in range(local)
    ) * (1.0 / route_scale)
    grads = jnp.concatenate(
        [
            meta_ref[l, 1] * (1.0 - meta_ref[l, 0]) * (scores[l] - mean)
            for l in range(local)
        ],
        axis=0,
    ).astype(jnp.bfloat16)
    out_ref[...] = contract_rows(grads, w_ref[...])[:tokens].astype(jnp.bfloat16)


def cost(flops, nbytes):
    return pl.CostEstimate(flops=flops, bytes_accessed=nbytes, transcendentals=0)


def struct(shape, dtype):
    return jax.ShapeDtypeStruct(shape, dtype)


def held(x):
    return pltpu.with_memory_space_constraint(x, pltpu.VMEM)


def away_from_vmem(x):
    return pltpu.with_memory_space_constraint(x, pltpu.HBM)


def kept(shape, dtype):
    return pltpu.VMEM(shape, dtype)


def token_plan(out_grad, expert_ids, router_logits, router_weight, expert_weight, hidden_saved):
    group_rows, features = out_grad.shape
    groups, ep_count = lax.axis_size("grp"), lax.axis_size("ep")
    local, _, width = expert_weight.shape
    slot_count = hidden_saved.shape[1]
    capacity = slot_count // (local * groups)
    span = groups * capacity
    tokens = groups * group_rows
    bf16, f32 = jnp.bfloat16, jnp.float32
    vmem = pl.BlockSpec(memory_space=pltpu.VMEM)
    hbm = pl.BlockSpec(memory_space=pltpu.HBM)

    def limit(mib):
        return pltpu.CompilerParams(vmem_limit_bytes=mib * 2**20)

    packed, meta = pl.pallas_call(
        functools.partial(pack_kernel, local),
        out_shape=(
            pltpu.VMEM((group_rows, features + LANES), bf16),
            pltpu.VMEM((local, 3, groups, LANES), f32),
        ),
        in_specs=[hbm] * 3,
        out_specs=(vmem, vmem),
        scratch_shapes=[
            pltpu.VMEM(expert_ids.shape[::-1], jnp.int32),
            pltpu.VMEM(router_logits.shape[::-1], f32),
            pltpu.SemaphoreType.DMA((3,)),
        ],
        compiler_params=limit(2),
        name="pack",
    )(away_from_vmem(expert_ids.T), away_from_vmem(router_logits.T), away_from_vmem(out_grad))
    blocks = [held(b) for b in gather_blocks(packed)]

    saved_shape = (local, groups // 2, 2, capacity, width)
    sums = [kept((local, span // 4, width), bf16)] * 2
    work = slot_count * features * width
    weights, saved, projection = pl.pallas_call(
        load_kernel,
        out_shape=(
            kept(expert_weight.shape, bf16),
            kept(saved_shape, bf16),
            kept(router_weight.shape, bf16),
        ),
        in_specs=[vmem] + [hbm] * 3,
        out_specs=(vmem,) * 3,
        scratch_shapes=[pltpu.SemaphoreType.DMA((3,))],
        compiler_params=limit(2),
        cost_estimate=cost(work // 2, 8 * 2**20),
        name="load",
    )(
        blocks[0],
        away_from_vmem(expert_weight),
        away_from_vmem(hidden_saved.reshape(saved_shape)),
        away_from_vmem(router_weight),
    )

    core_pairs = [(i, i ^ 1) for i in range(ep_count)]
    chip_pairs = [(i, i ^ 2) for i in range(ep_count)]

    def summed(kernel, keep, got):
        return pl.pallas_call(
            kernel,
            out_shape=(kept((span // 4, width), f32), kept((span // 4, width), bf16)),
            in_specs=[vmem] * 2,
            out_specs=(vmem,) * 2,
            compiler_params=limit(2),
        )(held(keep), held(got))

    keep_a, send_a, score_a = pl.pallas_call(
        functools.partial(first_kernel, groups, capacity),
        out_shape=(
            kept((span // 2, width), bf16),
            kept((span // 2, width), bf16),
            kept((groups // 2, LANES), f32),
        ),
        in_specs=[vmem] * (groups // 2 + 2),
        out_specs=(vmem,) * 3,
        compiler_params=limit(8),
        cost_estimate=cost(work, 4 * 2**20),
        name="first",
    )(*blocks[0::2], held(weights), held(saved))
    got_a = lax.ppermute(send_a, "ep", chip_pairs)

    keep_b, send_b, score = pl.pallas_call(
        functools.partial(second_kernel, local, groups, capacity),
        out_shape=(*sums, kept((groups // 2, 2, ep_count, LANES), f32)),
        in_specs=[vmem] * (groups // 2 + 3),
        out_specs=(vmem,) * 3,
        compiler_params=limit(8),
        cost_estimate=cost(work, 4 * 2**20),
        name="second",
    )(*blocks[1::2], held(weights), held(saved), held(score_a))
    got_b = lax.ppermute(send_b, "ep", core_pairs)
    from_all = lax.all_to_all(
        score.reshape(groups * ep_count, 1, LANES), ("grp", "ep"), 0, 0, tiled=True
    )
    mine_b, away_b = summed(pair_kernel, keep_b, got_b)
    last_b = lax.ppermute(away_b, "ep", chip_pairs)
    mine_a, away_a = summed(split_kernel, keep_a, got_a)
    last_a = lax.ppermute(away_a, "ep", core_pairs)

    parts = 4
    weight_grad, projection = pl.pallas_call(
        functools.partial(weight_kernel, local, groups, capacity, parts),
        out_shape=(struct((local, features, width), bf16), kept(router_weight.shape, bf16)),
        in_specs=[vmem] * (groups + 2),
        out_specs=(hbm, vmem),
        scratch_shapes=[
            pltpu.VMEM((features, tokens), bf16),
            pltpu.VMEM((features, span), bf16),
            pltpu.VMEM((local, features, width), bf16),
            pltpu.SemaphoreType.DMA((local * parts,)),
        ],
        compiler_params=limit(12),
        cost_estimate=cost(2 * slot_count * features * width, 6 * 2**20),
        name="weight",
    )(*blocks, held(saved.reshape(local, span, width)), held(projection))

    hidden_grad = pl.pallas_call(
        last_kernel,
        out_shape=struct((groups // 4, 2, capacity, width), bf16),
        in_specs=[vmem] * 4,
        out_specs=vmem,
        compiler_params=limit(2),
        name="last",
    )(held(mine_a), held(last_a), held(mine_b), held(last_b)).reshape(1, span // 2, width)

    input_grad = pl.pallas_call(
        functools.partial(router_kernel, local, capacity),
        out_shape=struct((group_rows, features), bf16),
        in_specs=[vmem] * 3,
        out_specs=vmem,
        compiler_params=limit(2),
        name="router",
    )(held(from_all.reshape(groups, ep_count, LANES)), held(meta), held(projection))
    return (weight_grad, hidden_grad, input_grad)


def body(out_grad, expert_ids, router_logits, router_weight, expert_weight, hidden_saved):
    groups, ep_count = lax.axis_size("grp"), lax.axis_size("ep")
    rows, experts = router_logits.shape
    slots = hidden_saved.shape[1]
    local = expert_weight.shape[0]
    fits = (
        rows * groups <= slots
        and groups % 8 == 0
        and groups & (groups - 1) == 0
        and (local, ep_count) == (2, 4)
        and rows % 16 == 0
        and slots // groups <= LANES
        and 2 * experts <= LANES
    )
    plan = token_plan if fits else slot_plan
    return plan(
        out_grad, expert_ids, router_logits, router_weight, expert_weight, hidden_saved
    )


def solution(mesh):
    in_specs = (
        P("grp", "ep"),
        P("grp", None),
        P("grp", None),
        P(None, "ep"),
        P("grp", "ep", None),
        P("grp", None, None),
    )
    out_specs = (P("grp", "ep", None), P("grp", "ep", None), P("grp", "ep"))
    return jax.shard_map(body, mesh=mesh, in_specs=in_specs, out_specs=out_specs, check_vma=False)
```

```python
import functools

import jax
import jax.numpy as jnp
from jax import lax
from jax.experimental import pallas as pl
from jax.experimental.pallas import tpu as pltpu
from jax.sharding import PartitionSpec as P


route_scale = 2.5
LANES = 128


def slot_plan(out_grad, expert_ids, router_logits, router_weight, expert_weight, hidden_saved):
    group_rows, features = out_grad.shape
    top_count = expert_ids.shape[1]
    experts = router_logits.shape[1]
    group_count = lax.axis_size("grp")
    local_experts = expert_weight.shape[0]
    hidden_width = expert_weight.shape[2]
    slot_count = hidden_saved.shape[1]
    capacity = slot_count // (local_experts * group_count)
    expert_span = group_count * capacity
    pair_count = group_rows * top_count
    sig_values = jax.nn.sigmoid(router_logits)
    picked = expert_ids[:, :, None] == jnp.arange(experts, dtype=jnp.int32)[None, None, :]
    chosen = jnp.sum(jnp.where(picked, sig_values[:, None, :], 0.0), axis=2)
    route_probs = route_scale * chosen / jnp.sum(chosen, axis=1, keepdims=True)
    flat_ids = expert_ids.reshape(pair_count)
    onehot = picked.reshape(pair_count, experts).astype(jnp.int32)
    pair_ranks = jnp.sum((jnp.cumsum(onehot, axis=0) - 1) * onehot, axis=1)
    slot_place = (
        flat_ids % local_experts * group_count + flat_ids // local_experts
    ) * capacity + pair_ranks
    slot_match = slot_place[None, :] == jnp.arange(slot_count, dtype=jnp.int32)[:, None]
    token_pick = jnp.sum(
        slot_match.reshape(slot_count, group_rows, top_count).astype(jnp.float32), axis=2
    ).astype(jnp.bfloat16)
    send_rows = jnp.dot(token_pick, out_grad, preferred_element_type=jnp.float32).astype(
        jnp.bfloat16
    )
    send_prob = jnp.sum(
        jnp.where(slot_match, route_probs.reshape(1, pair_count), 0.0), axis=1
    ).astype(jnp.bfloat16)
    swap = dict(split_axis=1, concat_axis=1, tiled=True)
    shape = (local_experts, group_count, capacity)
    got_rows = lax.all_to_all(send_rows.reshape(shape + (features,)), "grp", **swap)
    got_prob = lax.all_to_all(send_prob.reshape(shape), "grp", **swap)
    slot_grads = got_rows.reshape(local_experts, expert_span, features)
    prob_rows = got_prob.reshape(local_experts, expert_span).astype(jnp.float32)
    saved_rows = hidden_saved.reshape(local_experts, expert_span, hidden_width)
    scaled_rows = (prob_rows[:, :, None] * slot_grads.astype(jnp.float32)).astype(jnp.bfloat16)
    weight_grad = jnp.einsum(
        "lmd,lmf->ldf", scaled_rows, saved_rows, preferred_element_type=jnp.float32
    ).astype(jnp.bfloat16)
    owner_index = lax.axis_index("ep")
    share_rows = slot_count // lax.axis_size("ep")
    flat_prob = prob_rows.reshape(slot_count)
    flat_saved = hidden_saved.reshape(slot_count, hidden_width)
    partial_term = jnp.einsum(
        "lmd,ldf->lmf", slot_grads, expert_weight, preferred_element_type=jnp.float32
    ).reshape(slot_count, hidden_width)
    rounded_term = lax.optimization_barrier(partial_term.astype(jnp.bfloat16)).astype(jnp.float32)
    partial_score = jnp.sum(flat_saved.astype(jnp.float32) * rounded_term, axis=1)
    moved_scores = lax.all_to_all(partial_score.reshape(shape), "grp", **swap)
    returned = lax.psum(moved_scores, "ep")
    summed = lax.psum_scatter(
        partial_term.astype(jnp.bfloat16), "ep", scatter_dimension=0, tiled=True
    ).astype(jnp.float32)
    own_prob = lax.dynamic_slice_in_dim(flat_prob, owner_index * share_rows, share_rows, 0)
    hidden_grad = (own_prob[:, None] * summed).astype(jnp.bfloat16)[None]
    pair_score = jnp.sum(
        jnp.where(slot_match, returned.reshape(slot_count, 1), 0.0), axis=0
    ).reshape(group_rows, top_count)
    weighted_mean = jnp.sum(route_probs * pair_score, axis=1, keepdims=True) / route_scale
    logit_terms = route_probs * (1.0 - chosen) * (pair_score - weighted_mean)
    router_grad = jnp.sum(jnp.where(picked, logit_terms[:, :, None], 0.0), axis=1).astype(
        jnp.bfloat16
    )
    input_grad = jnp.dot(router_grad, router_weight, preferred_element_type=jnp.float32).astype(
        jnp.bfloat16
    )
    return (weight_grad, hidden_grad, input_grad)


def exchange(x, distance):
    count = lax.axis_size("grp")
    return lax.ppermute(x, "grp", [(i, i ^ distance) for i in range(count)])


def swap_order(count):
    far = list(range(count - 2, 0, -2))
    return far[:-1] + [1, 2, far[0] ^ 1, 3] + [d ^ 1 for d in far[1:-1]]


def gather_blocks(x):
    count = lax.axis_size("grp")
    blocks = {0: x}
    for distance in swap_order(count):
        if distance == 3:
            source, step = 1, 2
        else:
            source, step = (distance ^ 1, 1) if distance & 1 else (0, distance)
        blocks[distance] = exchange(blocks[source], step)
    return [blocks[d] for d in range(count)]


def iota(shape, dim):
    return lax.broadcasted_iota(jnp.int32, shape, dim)


def contract_rows(a, b):
    return lax.dot_general(a, b, (((0,), (0,)), ((), ())), preferred_element_type=jnp.float32)


def pack_kernel(local, ids_hbm, logits_hbm, rows_hbm, packed_ref, meta_ref, ids_ref, logits_ref, sems):
    top_count, tokens = ids_ref.shape
    groups = logits_ref.shape[0] // local
    features = rows_hbm.shape[1]
    copies = [
        pltpu.make_async_copy(ids_hbm, ids_ref, sems.at[0]),
        pltpu.make_async_copy(logits_hbm, logits_ref, sems.at[1]),
        pltpu.make_async_copy(rows_hbm, packed_ref.at[:, pl.ds(0, features)], sems.at[2]),
    ]
    for c in copies:
        c.start()
    copies[0].wait()
    copies[1].wait()
    ids = ids_ref[...]
    upto = (iota((tokens, tokens), 0) <= iota((tokens, tokens), 1)).astype(jnp.bfloat16)
    named, sig, chosen, ranks = [], [], [], []
    for l in range(local):
        expert = iota((groups, tokens), 0) * local + l
        hit = jnp.zeros((groups, tokens), jnp.float32)
        for i in range(top_count):
            hit = hit + (ids[i : i + 1, :] == expert).astype(jnp.float32)
        value = jax.nn.sigmoid(logits_ref[pl.ds(l, groups, stride=local), :])
        named.append(hit)
        sig.append(value)
        chosen.append(hit * value)
        count = jnp.dot(hit.astype(jnp.bfloat16), upto, preferred_element_type=jnp.float32)
        ranks.append(hit * count)
    total = sum(jnp.sum(c, axis=0, keepdims=True) for c in chosen)
    probs = [route_scale * c / total for c in chosen]
    lanes = packed_ref.shape[1] - features
    count = local * groups
    rest = jnp.zeros((lanes - 2 * count, tokens), jnp.float32)
    none = jnp.zeros((count, tokens), jnp.float32)
    table = jnp.concatenate(
        [
            jnp.concatenate(probs + [none, rest], axis=0),
            jnp.concatenate([none] + named + [rest], axis=0),
        ],
        axis=1,
    ).astype(jnp.bfloat16)
    at, of = iota((tokens, 2 * tokens), 0), iota((tokens, 2 * tokens), 1)
    weigh = ((of == at) | ((of >= tokens) & (of - tokens <= at))).astype(jnp.bfloat16)
    packed_ref[:, features:] = lax.dot_general(
        weigh, table, (((1,), (1,)), ((), ())), preferred_element_type=jnp.float32
    ).astype(jnp.bfloat16)
    for l in range(local):
        for k, value in enumerate((sig[l], probs[l], ranks[l])):
            meta_ref[l, k] = jnp.zeros(meta_ref.shape[2:], jnp.float32)
            meta_ref[l, k, :, :tokens] = value
    copies[2].wait()


def half_of(parity, experts, groups, capacity, blocks, saved_ref, w_ref, store, ready=None):
    local = len(experts)
    block_rows, features = blocks[0].shape[0], blocks[0].shape[1] - LANES
    width = w_ref.shape[2]
    count = groups // 2
    span, tokens = count * capacity, count * block_rows
    cols = 256 if width % 256 == 0 else LANES
    own, side = lax.axis_index("grp"), lax.rem(lax.axis_index("ep"), 2)
    rows = jnp.concatenate([b[:, :features] for b in blocks], axis=0)
    aux = jnp.concatenate([b[:, features:] for b in blocks], axis=0).astype(jnp.float32).T
    source = (iota((1, tokens), 1) // block_rows) ^ (own // 2)
    slot = iota((span, tokens), 0) + side * (span // 2)
    slot = jnp.where(slot >= span, slot - span, slot)
    near = pl.ds(side * (count // 2), count // 2)
    away = pl.ds((1 - side) * (count // 2), count // 2)
    part_row, part_lane = iota((span, LANES), 0), iota((span, LANES), 1)
    sent = jnp.zeros((count, LANES), jnp.float32)
    row = iota(aux.shape, 0)
    picks, scales = [], []
    for l in experts:
        lane = l * groups + own
        prob = jnp.sum(jnp.where(row == lane, aux, 0.0), axis=0, keepdims=True)
        rank = jnp.sum(jnp.where(row == local * groups + lane, aux, 0.0), axis=0, keepdims=True)
        place = jnp.where(prob > 0, source * capacity + rank.astype(jnp.int32) - 1, -1)
        pick = slot == place
        picks.append(pick.astype(jnp.float32).astype(jnp.bfloat16))
        scales.append(jnp.sum(jnp.where(pick, prob, 0.0), axis=1, keepdims=True))
    grads = jnp.dot(
        jnp.concatenate(picks, axis=0), rows, preferred_element_type=jnp.float32
    ).astype(jnp.bfloat16)
    if ready is not None:
        ready()
    for i, l in enumerate(experts):
        score = jnp.zeros((span, LANES), jnp.float32)
        for n in range(width // cols):
            part = pl.ds(n * cols, cols)
            term = jnp.dot(
                grads[i * span : (i + 1) * span],
                w_ref[l, :, part],
                preferred_element_type=jnp.float32,
            )
            saved = jnp.concatenate(
                [
                    saved_ref[l, where, parity, :, part].reshape(span // 2, cols)
                    for where in (near, away)
                ],
                axis=0,
            )
            product = term * saved.astype(jnp.float32)
            for k in range(cols // LANES):
                score = score + product[:, k * LANES : (k + 1) * LANES]
            store(i, part, (term * scales[i]).astype(jnp.bfloat16))
        score = jnp.sum(score, axis=1, keepdims=True)
        spread = jnp.where(lax.rem(part_row, capacity) + l * capacity == part_lane, score, 0.0)
        sent = sent + jnp.sum(spread.reshape(count, capacity, LANES), axis=1)
    turned = jnp.concatenate([sent[count // 2 :], sent[: count // 2]], axis=0)
    return jnp.where(side == 0, sent, turned)


def load_kernel(cue_ref, source_ref, out_ref, sems):
    copies = [
        pltpu.make_async_copy(source_ref.at[i], out_ref.at[i], sems.at[i])
        for i in range(source_ref.shape[0])
    ]
    for copy in copies:
        copy.start()
    for copy in copies:
        copy.wait()


def first_kernel(groups, capacity, *refs):
    count = groups // 2
    blocks = refs[:count]
    w_ref, *sources = refs[count : count + 3]
    h_ref, r_ref, keep_ref, send_ref, score_ref, sems = refs[count + 3 :]
    bit = lax.axis_index("ep") // 2
    copies = [
        pltpu.make_async_copy(source, target, sems.at[i])
        for i, (source, target) in enumerate(zip(sources, (h_ref, r_ref)))
    ]
    for copy in copies:
        copy.start()

    def store(i, part, value):
        (send_ref, keep_ref)[i][:, part] = value

    score_ref[...] = half_of(
        lax.rem(lax.axis_index("grp"), 2),
        (1 - bit, bit),
        groups,
        capacity,
        blocks,
        h_ref,
        w_ref,
        store,
        copies[0].wait,
    )
    copies[1].wait()


def second_kernel(local, groups, capacity, *refs):
    count = groups // 2
    blocks = refs[:count]
    w_ref, h_ref, other_ref, keep_ref, send_ref, score_ref = refs[count:]
    parity = 1 - lax.rem(lax.axis_index("grp"), 2)
    rows = keep_ref.shape[1]

    def store(l, part, value):
        keep_ref[l, :, part] = value[:rows]
        send_ref[l, :, part] = value[rows:]

    mine = half_of(
        parity, tuple(range(local)), groups, capacity, blocks, h_ref, w_ref, store
    )
    other = other_ref[...]
    for x in range(2):
        value = jnp.where(parity == x, mine, other)
        score_ref[:, x] = jnp.broadcast_to(
            value[:, None, :], (count,) + score_ref.shape[2:]
        )


def weight_kernel(local, groups, capacity, parts, *refs):
    blocks = refs[:groups]
    h_ref, r_ref, out_hbm, sorted_ref, turned_buf, scaled_buf, out_buf, sems = refs[groups:]
    experts = r_ref.shape[0]
    at = iota((experts, experts), 0)
    order = lax.rem(at, groups) * local + at // groups == iota((experts, experts), 1)
    sorted_ref[...] = jnp.dot(
        order.astype(jnp.float32).astype(jnp.bfloat16), r_ref[...], preferred_element_type=jnp.float32
    ).astype(jnp.bfloat16)
    features = turned_buf.shape[0]
    tile = features // parts
    block_rows = blocks[0].shape[0]
    span = groups * capacity
    tokens = groups * block_rows
    own = lax.axis_index("grp")
    rows = jnp.concatenate([b[:, :features] for b in blocks], axis=0)
    turned_buf[...] = rows.T
    aux = jnp.concatenate([b[:, features:] for b in blocks], axis=0).astype(jnp.float32)
    at = iota(aux.shape, 1)
    source = (iota((tokens, 1), 0) // block_rows) ^ own
    copies = []
    for l in range(local):
        lane = l * groups + own
        prob = jnp.sum(jnp.where(at == lane, aux, 0.0), axis=1, keepdims=True)
        rank = jnp.sum(jnp.where(at == local * groups + lane, aux, 0.0), axis=1, keepdims=True)
        place = jnp.where(prob > 0, source * capacity + rank.astype(jnp.int32) - 1, -1)
        pick = jnp.where(place == iota((tokens, span), 1), prob, 0.0).astype(jnp.bfloat16)
        scaled_buf[...] = jnp.dot(
            turned_buf[...], pick, preferred_element_type=jnp.float32
        ).astype(jnp.bfloat16)
        for d in range(parts):
            part = pl.ds(d * tile, tile)
            out_buf[l, part] = jnp.dot(
                scaled_buf[part], h_ref[l], preferred_element_type=jnp.float32
            ).astype(jnp.bfloat16)
            copy = pltpu.make_async_copy(
                out_buf.at[l, part], out_hbm.at[l, part], sems.at[l * parts + d]
            )
            copy.start()
            copies.append(copy)
    for copy in copies:
        copy.wait()


def pair_kernel(mine_ref, got_ref, keep_ref, send_ref):
    bit = lax.axis_index("ep") // 2
    keep_ref[...] = mine_ref[bit].astype(jnp.float32) + got_ref[bit].astype(jnp.float32)
    send_ref[...] = (
        mine_ref[1 - bit].astype(jnp.float32) + got_ref[1 - bit].astype(jnp.float32)
    ).astype(jnp.bfloat16)


def split_kernel(mine_ref, got_ref, keep_ref, send_ref):
    rows = keep_ref.shape[0]
    total = mine_ref[...].astype(jnp.float32) + got_ref[...].astype(jnp.float32)
    keep_ref[...] = total[:rows]
    send_ref[...] = total[rows:].astype(jnp.bfloat16)


def last_kernel(mine_a, got_a, mine_b, got_b, out_ref):
    parity = lax.rem(lax.axis_index("grp"), 2)
    shape = out_ref.shape[:1] + out_ref.shape[2:]
    for at, mine, got in ((parity, mine_a, got_a), (1 - parity, mine_b, got_b)):
        total = mine[...] + got[...].astype(jnp.float32)
        out_ref[:, at] = total.astype(jnp.bfloat16).reshape(shape)


def router_kernel(local, capacity, score_ref, meta_ref, w_ref, out_ref):
    tokens = out_ref.shape[0]
    found = jnp.sum(score_ref[...], axis=1)
    scores = []
    for l in range(local):
        rank = meta_ref[l, 2].astype(jnp.int32)
        at = jnp.maximum(rank + (l * capacity - 1), 0)
        value = jnp.take_along_axis(found, at, axis=1, mode="promise_in_bounds")
        scores.append(jnp.where(rank > 0, value, 0.0))
    mean = sum(
        jnp.sum(meta_ref[l, 1] * scores[l], axis=0, keepdims=True) for l in range(local)
    ) * (1.0 / route_scale)
    grads = jnp.concatenate(
        [
            meta_ref[l, 1] * (1.0 - meta_ref[l, 0]) * (scores[l] - mean)
            for l in range(local)
        ],
        axis=0,
    ).astype(jnp.bfloat16)
    out_ref[...] = contract_rows(grads, w_ref[...])[:tokens].astype(jnp.bfloat16)


def cost(flops, nbytes):
    return pl.CostEstimate(flops=flops, bytes_accessed=nbytes, transcendentals=0)


def struct(shape, dtype):
    return jax.ShapeDtypeStruct(shape, dtype)


def held(x):
    return pltpu.with_memory_space_constraint(x, pltpu.VMEM)


def away_from_vmem(x):
    return pltpu.with_memory_space_constraint(x, pltpu.HBM)


def kept(shape, dtype):
    return pltpu.VMEM(shape, dtype)


def token_plan(out_grad, expert_ids, router_logits, router_weight, expert_weight, hidden_saved):
    group_rows, features = out_grad.shape
    groups, ep_count = lax.axis_size("grp"), lax.axis_size("ep")
    local, _, width = expert_weight.shape
    slot_count = hidden_saved.shape[1]
    capacity = slot_count // (local * groups)
    span = groups * capacity
    tokens = groups * group_rows
    bf16, f32 = jnp.bfloat16, jnp.float32
    vmem = pl.BlockSpec(memory_space=pltpu.VMEM)
    hbm = pl.BlockSpec(memory_space=pltpu.HBM)

    def limit(mib):
        return pltpu.CompilerParams(vmem_limit_bytes=mib * 2**20)

    packed, meta = pl.pallas_call(
        functools.partial(pack_kernel, local),
        out_shape=(
            pltpu.VMEM((group_rows, features + LANES), bf16),
            pltpu.VMEM((local, 3, groups, LANES), f32),
        ),
        in_specs=[hbm] * 3,
        out_specs=(vmem, vmem),
        scratch_shapes=[
            pltpu.VMEM(expert_ids.shape[::-1], jnp.int32),
            pltpu.VMEM(router_logits.shape[::-1], f32),
            pltpu.SemaphoreType.DMA((3,)),
        ],
        compiler_params=limit(2),
        name="pack",
    )(away_from_vmem(expert_ids.T), away_from_vmem(router_logits.T), away_from_vmem(out_grad))
    blocks = [held(b) for b in gather_blocks(packed)]

    saved_shape = (local, groups // 2, 2, capacity, width)
    sums = [kept((local, span // 4, width), bf16)] * 2
    work = slot_count * features * width
    weights = pl.pallas_call(
        load_kernel,
        out_shape=kept(expert_weight.shape, bf16),
        in_specs=[vmem, hbm],
        out_specs=vmem,
        scratch_shapes=[pltpu.SemaphoreType.DMA((local,))],
        compiler_params=limit(2),
        cost_estimate=cost(work // 2, 8 * 2**20),
        name="load",
    )(blocks[0], away_from_vmem(expert_weight))

    core_pairs = [(i, i ^ 1) for i in range(ep_count)]
    chip_pairs = [(i, i ^ 2) for i in range(ep_count)]

    def summed(kernel, keep, got):
        return pl.pallas_call(
            kernel,
            out_shape=(kept((span // 4, width), f32), kept((span // 4, width), bf16)),
            in_specs=[vmem] * 2,
            out_specs=(vmem,) * 2,
            compiler_params=limit(2),
        )(held(keep), held(got))

    saved, projection, keep_a, send_a, score_a = pl.pallas_call(
        functools.partial(first_kernel, groups, capacity),
        out_shape=(
            kept(saved_shape, bf16),
            kept(router_weight.shape, bf16),
            kept((span // 2, width), bf16),
            kept((span // 2, width), bf16),
            kept((groups // 2, LANES), f32),
        ),
        in_specs=[vmem] * (groups // 2 + 1) + [hbm] * 2,
        out_specs=(vmem,) * 5,
        scratch_shapes=[pltpu.SemaphoreType.DMA((2,))],
        compiler_params=limit(8),
        cost_estimate=cost(work, 4 * 2**20),
        name="first",
    )(
        *blocks[0::2],
        held(weights),
        away_from_vmem(hidden_saved.reshape(saved_shape)),
        away_from_vmem(router_weight),
    )
    got_a = lax.ppermute(send_a, "ep", chip_pairs)

    keep_b, send_b, score = pl.pallas_call(
        functools.partial(second_kernel, local, groups, capacity),
        out_shape=(*sums, kept((groups // 2, 2, ep_count, LANES), f32)),
        in_specs=[vmem] * (groups // 2 + 3),
        out_specs=(vmem,) * 3,
        compiler_params=limit(8),
        cost_estimate=cost(work, 4 * 2**20),
        name="second",
    )(*blocks[1::2], held(weights), held(saved), held(score_a))
    got_b = lax.ppermute(send_b, "ep", core_pairs)
    from_all = lax.all_to_all(
        score.reshape(groups * ep_count, 1, LANES), ("grp", "ep"), 0, 0, tiled=True
    )
    mine_b, away_b = summed(pair_kernel, keep_b, got_b)
    last_b = lax.ppermute(away_b, "ep", chip_pairs)
    mine_a, away_a = summed(split_kernel, keep_a, got_a)
    last_a = lax.ppermute(away_a, "ep", core_pairs)

    parts = 4
    weight_grad, projection = pl.pallas_call(
        functools.partial(weight_kernel, local, groups, capacity, parts),
        out_shape=(struct((local, features, width), bf16), kept(router_weight.shape, bf16)),
        in_specs=[vmem] * (groups + 2),
        out_specs=(hbm, vmem),
        scratch_shapes=[
            pltpu.VMEM((features, tokens), bf16),
            pltpu.VMEM((features, span), bf16),
            pltpu.VMEM((local, features, width), bf16),
            pltpu.SemaphoreType.DMA((local * parts,)),
        ],
        compiler_params=limit(12),
        cost_estimate=cost(2 * slot_count * features * width, 6 * 2**20),
        name="weight",
    )(*blocks, held(saved.reshape(local, span, width)), held(projection))

    hidden_grad = pl.pallas_call(
        last_kernel,
        out_shape=struct((groups // 4, 2, capacity, width), bf16),
        in_specs=[vmem] * 4,
        out_specs=vmem,
        compiler_params=limit(2),
        name="last",
    )(held(mine_a), held(last_a), held(mine_b), held(last_b)).reshape(1, span // 2, width)

    input_grad = pl.pallas_call(
        functools.partial(router_kernel, local, capacity),
        out_shape=struct((group_rows, features), bf16),
        in_specs=[vmem] * 3,
        out_specs=vmem,
        compiler_params=limit(2),
        name="router",
    )(held(from_all.reshape(groups, ep_count, LANES)), held(meta), held(projection))
    return (weight_grad, hidden_grad, input_grad)


def body(out_grad, expert_ids, router_logits, router_weight, expert_weight, hidden_saved):
    groups, ep_count = lax.axis_size("grp"), lax.axis_size("ep")
    rows, experts = router_logits.shape
    slots = hidden_saved.shape[1]
    local = expert_weight.shape[0]
    fits = (
        rows * groups <= slots
        and groups % 8 == 0
        and groups & (groups - 1) == 0
        and (local, ep_count) == (2, 4)
        and rows % 16 == 0
        and slots // groups <= LANES
        and 2 * experts <= LANES
    )
    plan = token_plan if fits else slot_plan
    return plan(
        out_grad, expert_ids, router_logits, router_weight, expert_weight, hidden_saved
    )


def solution(mesh):
    in_specs = (
        P("grp", "ep"),
        P("grp", None),
        P("grp", None),
        P(None, "ep"),
        P("grp", "ep", None),
        P("grp", None, None),
    )
    out_specs = (P("grp", "ep", None), P("grp", "ep", None), P("grp", "ep"))
    return jax.shard_map(body, mesh=mesh, in_specs=in_specs, out_specs=out_specs, check_vma=False)
```

```python
import functools

import jax
import jax.numpy as jnp
from jax import lax
from jax.experimental import pallas as pl
from jax.experimental.pallas import tpu as pltpu
from jax.sharding import PartitionSpec as P


route_scale = 2.5
LANES = 128


def slot_plan(out_grad, expert_ids, router_logits, router_weight, expert_weight, hidden_saved):
    group_rows, features = out_grad.shape
    top_count = expert_ids.shape[1]
    experts = router_logits.shape[1]
    group_count = lax.axis_size("grp")
    local_experts = expert_weight.shape[0]
    hidden_width = expert_weight.shape[2]
    slot_count = hidden_saved.shape[1]
    capacity = slot_count // (local_experts * group_count)
    expert_span = group_count * capacity
    pair_count = group_rows * top_count
    sig_values = jax.nn.sigmoid(router_logits)
    picked = expert_ids[:, :, None] == jnp.arange(experts, dtype=jnp.int32)[None, None, :]
    chosen = jnp.sum(jnp.where(picked, sig_values[:, None, :], 0.0), axis=2)
    route_probs = route_scale * chosen / jnp.sum(chosen, axis=1, keepdims=True)
    flat_ids = expert_ids.reshape(pair_count)
    onehot = picked.reshape(pair_count, experts).astype(jnp.int32)
    pair_ranks = jnp.sum((jnp.cumsum(onehot, axis=0) - 1) * onehot, axis=1)
    slot_place = (
        flat_ids % local_experts * group_count + flat_ids // local_experts
    ) * capacity + pair_ranks
    slot_match = slot_place[None, :] == jnp.arange(slot_count, dtype=jnp.int32)[:, None]
    token_pick = jnp.sum(
        slot_match.reshape(slot_count, group_rows, top_count).astype(jnp.float32), axis=2
    ).astype(jnp.bfloat16)
    send_rows = jnp.dot(token_pick, out_grad, preferred_element_type=jnp.float32).astype(
        jnp.bfloat16
    )
    send_prob = jnp.sum(
        jnp.where(slot_match, route_probs.reshape(1, pair_count), 0.0), axis=1
    ).astype(jnp.bfloat16)
    swap = dict(split_axis=1, concat_axis=1, tiled=True)
    shape = (local_experts, group_count, capacity)
    got_rows = lax.all_to_all(send_rows.reshape(shape + (features,)), "grp", **swap)
    got_prob = lax.all_to_all(send_prob.reshape(shape), "grp", **swap)
    slot_grads = got_rows.reshape(local_experts, expert_span, features)
    prob_rows = got_prob.reshape(local_experts, expert_span).astype(jnp.float32)
    saved_rows = hidden_saved.reshape(local_experts, expert_span, hidden_width)
    scaled_rows = (prob_rows[:, :, None] * slot_grads.astype(jnp.float32)).astype(jnp.bfloat16)
    weight_grad = jnp.einsum(
        "lmd,lmf->ldf", scaled_rows, saved_rows, preferred_element_type=jnp.float32
    ).astype(jnp.bfloat16)
    owner_index = lax.axis_index("ep")
    share_rows = slot_count // lax.axis_size("ep")
    flat_prob = prob_rows.reshape(slot_count)
    flat_saved = hidden_saved.reshape(slot_count, hidden_width)
    partial_term = jnp.einsum(
        "lmd,ldf->lmf", slot_grads, expert_weight, preferred_element_type=jnp.float32
    ).reshape(slot_count, hidden_width)
    rounded_term = lax.optimization_barrier(partial_term.astype(jnp.bfloat16)).astype(jnp.float32)
    partial_score = jnp.sum(flat_saved.astype(jnp.float32) * rounded_term, axis=1)
    moved_scores = lax.all_to_all(partial_score.reshape(shape), "grp", **swap)
    returned = lax.psum(moved_scores, "ep")
    summed = lax.psum_scatter(
        partial_term.astype(jnp.bfloat16), "ep", scatter_dimension=0, tiled=True
    ).astype(jnp.float32)
    own_prob = lax.dynamic_slice_in_dim(flat_prob, owner_index * share_rows, share_rows, 0)
    hidden_grad = (own_prob[:, None] * summed).astype(jnp.bfloat16)[None]
    pair_score = jnp.sum(
        jnp.where(slot_match, returned.reshape(slot_count, 1), 0.0), axis=0
    ).reshape(group_rows, top_count)
    weighted_mean = jnp.sum(route_probs * pair_score, axis=1, keepdims=True) / route_scale
    logit_terms = route_probs * (1.0 - chosen) * (pair_score - weighted_mean)
    router_grad = jnp.sum(jnp.where(picked, logit_terms[:, :, None], 0.0), axis=1).astype(
        jnp.bfloat16
    )
    input_grad = jnp.dot(router_grad, router_weight, preferred_element_type=jnp.float32).astype(
        jnp.bfloat16
    )
    return (weight_grad, hidden_grad, input_grad)


def exchange(x, distance):
    count = lax.axis_size("grp")
    return lax.ppermute(x, "grp", [(i, i ^ distance) for i in range(count)])


def swap_order(count):
    far = list(range(count - 2, 0, -2))
    return far[:1] + [1] + far[1:] + [3, far[0] ^ 1] + [d ^ 1 for d in far[1:-1]]


def gather_blocks(x):
    count = lax.axis_size("grp")
    blocks = {0: x}
    for distance in swap_order(count):
        if distance == 3:
            source, step = 1, 2
        else:
            source, step = (distance ^ 1, 1) if distance & 1 else (0, distance)
        blocks[distance] = exchange(blocks[source], step)
    return [blocks[d] for d in range(count)]


def iota(shape, dim):
    return lax.broadcasted_iota(jnp.int32, shape, dim)


def contract_rows(a, b):
    return lax.dot_general(a, b, (((0,), (0,)), ((), ())), preferred_element_type=jnp.float32)


def pack_kernel(local, ids_hbm, logits_hbm, rows_hbm, packed_ref, meta_ref, ids_ref, logits_ref, sems):
    top_count, tokens = ids_ref.shape
    groups = logits_ref.shape[0] // local
    features = rows_hbm.shape[1]
    copies = [
        pltpu.make_async_copy(ids_hbm, ids_ref, sems.at[0]),
        pltpu.make_async_copy(logits_hbm, logits_ref, sems.at[1]),
        pltpu.make_async_copy(rows_hbm, packed_ref.at[:, pl.ds(0, features)], sems.at[2]),
    ]
    for c in copies:
        c.start()
    copies[0].wait()
    copies[1].wait()
    ids = ids_ref[...]
    upto = (iota((tokens, tokens), 0) <= iota((tokens, tokens), 1)).astype(jnp.bfloat16)
    named, sig, chosen, ranks = [], [], [], []
    for l in range(local):
        expert = iota((groups, tokens), 0) * local + l
        hit = jnp.zeros((groups, tokens), jnp.float32)
        for i in range(top_count):
            hit = hit + (ids[i : i + 1, :] == expert).astype(jnp.float32)
        value = jax.nn.sigmoid(logits_ref[pl.ds(l, groups, stride=local), :])
        named.append(hit)
        sig.append(value)
        chosen.append(hit * value)
        count = jnp.dot(hit.astype(jnp.bfloat16), upto, preferred_element_type=jnp.float32)
        ranks.append(hit * count)
    total = sum(jnp.sum(c, axis=0, keepdims=True) for c in chosen)
    probs = [route_scale * c / total for c in chosen]
    lanes = packed_ref.shape[1] - features
    count = local * groups
    rest = jnp.zeros((lanes - 2 * count, tokens), jnp.float32)
    none = jnp.zeros((count, tokens), jnp.float32)
    table = jnp.concatenate(
        [
            jnp.concatenate(probs + [none, rest], axis=0),
            jnp.concatenate([none] + named + [rest], axis=0),
        ],
        axis=1,
    ).astype(jnp.bfloat16)
    at, of = iota((tokens, 2 * tokens), 0), iota((tokens, 2 * tokens), 1)
    weigh = ((of == at) | ((of >= tokens) & (of - tokens <= at))).astype(jnp.bfloat16)
    packed_ref[:, features:] = lax.dot_general(
        weigh, table, (((1,), (1,)), ((), ())), preferred_element_type=jnp.float32
    ).astype(jnp.bfloat16)
    for l in range(local):
        for k, value in enumerate((sig[l], probs[l], ranks[l])):
            meta_ref[l, k] = jnp.zeros(meta_ref.shape[2:], jnp.float32)
            meta_ref[l, k, :, :tokens] = value
    copies[2].wait()


def half_of(parity, experts, groups, capacity, blocks, saved_ref, w_ref, store, ready=None):
    local = len(experts)
    block_rows, features = blocks[0].shape[0], blocks[0].shape[1] - LANES
    width = w_ref.shape[2]
    count = groups // 2
    span, tokens = count * capacity, count * block_rows
    cols = 256 if width % 256 == 0 else LANES
    own, side = lax.axis_index("grp"), lax.rem(lax.axis_index("ep"), 2)
    rows = jnp.concatenate([b[:, :features] for b in blocks], axis=0)
    aux = jnp.concatenate([b[:, features:] for b in blocks], axis=0).astype(jnp.float32).T
    source = (iota((1, tokens), 1) // block_rows) ^ (own // 2)
    slot = iota((span, tokens), 0) + side * (span // 2)
    slot = jnp.where(slot >= span, slot - span, slot)
    near = pl.ds(side * (count // 2), count // 2)
    away = pl.ds((1 - side) * (count // 2), count // 2)
    part_row, part_lane = iota((span, LANES), 0), iota((span, LANES), 1)
    sent = jnp.zeros((count, LANES), jnp.float32)
    row = iota(aux.shape, 0)
    picks, scales = [], []
    for l in experts:
        lane = l * groups + own
        prob = jnp.sum(jnp.where(row == lane, aux, 0.0), axis=0, keepdims=True)
        rank = jnp.sum(jnp.where(row == local * groups + lane, aux, 0.0), axis=0, keepdims=True)
        place = jnp.where(prob > 0, source * capacity + rank.astype(jnp.int32) - 1, -1)
        pick = slot == place
        picks.append(pick.astype(jnp.float32).astype(jnp.bfloat16))
        scales.append(jnp.sum(jnp.where(pick, prob, 0.0), axis=1, keepdims=True))
    grads = jnp.dot(
        jnp.concatenate(picks, axis=0), rows, preferred_element_type=jnp.float32
    ).astype(jnp.bfloat16)
    for i, l in enumerate(experts):
        if ready is not None:
            ready(i)
        score = jnp.zeros((span, LANES), jnp.float32)
        for n in range(width // cols):
            part = pl.ds(n * cols, cols)
            term = jnp.dot(
                grads[i * span : (i + 1) * span],
                w_ref[l, :, part],
                preferred_element_type=jnp.float32,
            )
            saved = jnp.concatenate(
                [
                    saved_ref[l, where, parity, :, part].reshape(span // 2, cols)
                    for where in (near, away)
                ],
                axis=0,
            )
            product = term * saved.astype(jnp.float32)
            for k in range(cols // LANES):
                score = score + product[:, k * LANES : (k + 1) * LANES]
            store(i, part, (term * scales[i]).astype(jnp.bfloat16))
        score = jnp.sum(score, axis=1, keepdims=True)
        spread = jnp.where(lax.rem(part_row, capacity) + l * capacity == part_lane, score, 0.0)
        sent = sent + jnp.sum(spread.reshape(count, capacity, LANES), axis=1)
    turned = jnp.concatenate([sent[count // 2 :], sent[: count // 2]], axis=0)
    return jnp.where(side == 0, sent, turned)


def load_kernel(cue_ref, source_ref, saved_hbm, out_ref, saved_ref, sems):
    at = (slice(None), slice(None), lax.rem(lax.axis_index("grp"), 2))
    sent = 1 - lax.axis_index("ep") // 2
    copies = [
        pltpu.make_async_copy(source_ref.at[sent], out_ref.at[sent], sems.at[0]),
        pltpu.make_async_copy(saved_hbm.at[at], saved_ref.at[at], sems.at[1]),
    ]
    for copy in copies:
        copy.start()
    for copy in copies:
        copy.wait()


def first_kernel(groups, capacity, *refs):
    count = groups // 2
    blocks = refs[:count]
    w_hbm, saved_hbm, r_hbm = refs[count : count + 3]
    w_ref, h_ref, r_ref, keep_ref, send_ref, score_ref, sems = refs[count + 5 :]
    bit = lax.axis_index("ep") // 2
    parity = lax.rem(lax.axis_index("grp"), 2)
    experts = (1 - bit, bit)
    at = (slice(None), slice(None), 1 - parity)
    copies = [
        pltpu.make_async_copy(w_hbm.at[bit], w_ref.at[bit], sems.at[0]),
        pltpu.make_async_copy(saved_hbm.at[at], h_ref.at[at], sems.at[1]),
        pltpu.make_async_copy(r_hbm, r_ref, sems.at[2]),
    ]
    for copy in copies:
        copy.start()

    def store(i, part, value):
        (send_ref, keep_ref)[i][:, part] = value

    score_ref[...] = half_of(
        parity,
        experts,
        groups,
        capacity,
        blocks,
        h_ref,
        w_ref,
        store,
        lambda i: copies[0].wait() if i == 1 else None,
    )
    for copy in copies[1:]:
        copy.wait()


def second_kernel(local, groups, capacity, *refs):
    count = groups // 2
    blocks = refs[:count]
    w_ref, h_ref, other_ref, keep_ref, send_ref, score_ref = refs[count:]
    parity = 1 - lax.rem(lax.axis_index("grp"), 2)
    rows = keep_ref.shape[1]

    def store(l, part, value):
        keep_ref[l, :, part] = value[:rows]
        send_ref[l, :, part] = value[rows:]

    mine = half_of(
        parity, tuple(range(local)), groups, capacity, blocks, h_ref, w_ref, store
    )
    other = other_ref[...]
    for x in range(2):
        value = jnp.where(parity == x, mine, other)
        score_ref[:, x] = jnp.broadcast_to(
            value[:, None, :], (count,) + score_ref.shape[2:]
        )


def weight_kernel(local, groups, capacity, parts, *refs):
    blocks = refs[:groups]
    h_ref, r_ref, out_hbm, sorted_ref, turned_buf, scaled_buf, out_buf, sems = refs[groups:]
    experts = r_ref.shape[0]
    at = iota((experts, experts), 0)
    order = lax.rem(at, groups) * local + at // groups == iota((experts, experts), 1)
    sorted_ref[...] = jnp.dot(
        order.astype(jnp.float32).astype(jnp.bfloat16), r_ref[...], preferred_element_type=jnp.float32
    ).astype(jnp.bfloat16)
    features = turned_buf.shape[0]
    tile = features // parts
    block_rows = blocks[0].shape[0]
    span = groups * capacity
    tokens = groups * block_rows
    own = lax.axis_index("grp")
    rows = jnp.concatenate([b[:, :features] for b in blocks], axis=0)
    turned_buf[...] = rows.T
    aux = jnp.concatenate([b[:, features:] for b in blocks], axis=0).astype(jnp.float32)
    at = iota(aux.shape, 1)
    source = (iota((tokens, 1), 0) // block_rows) ^ own
    copies = []
    for l in range(local):
        lane = l * groups + own
        prob = jnp.sum(jnp.where(at == lane, aux, 0.0), axis=1, keepdims=True)
        rank = jnp.sum(jnp.where(at == local * groups + lane, aux, 0.0), axis=1, keepdims=True)
        place = jnp.where(prob > 0, source * capacity + rank.astype(jnp.int32) - 1, -1)
        pick = jnp.where(place == iota((tokens, span), 1), prob, 0.0).astype(jnp.bfloat16)
        scaled_buf[...] = jnp.dot(
            turned_buf[...], pick, preferred_element_type=jnp.float32
        ).astype(jnp.bfloat16)
        for d in range(parts):
            part = pl.ds(d * tile, tile)
            out_buf[l, part] = jnp.dot(
                scaled_buf[part], h_ref[l], preferred_element_type=jnp.float32
            ).astype(jnp.bfloat16)
            copy = pltpu.make_async_copy(
                out_buf.at[l, part], out_hbm.at[l, part], sems.at[l * parts + d]
            )
            copy.start()
            copies.append(copy)
    for copy in copies:
        copy.wait()


def pair_kernel(mine_ref, got_ref, keep_ref, send_ref):
    bit = lax.axis_index("ep") // 2
    keep_ref[...] = mine_ref[bit].astype(jnp.float32) + got_ref[bit].astype(jnp.float32)
    send_ref[...] = (
        mine_ref[1 - bit].astype(jnp.float32) + got_ref[1 - bit].astype(jnp.float32)
    ).astype(jnp.bfloat16)


def split_kernel(mine_ref, got_ref, keep_ref, send_ref):
    rows = keep_ref.shape[0]
    total = mine_ref[...].astype(jnp.float32) + got_ref[...].astype(jnp.float32)
    keep_ref[...] = total[:rows]
    send_ref[...] = total[rows:].astype(jnp.bfloat16)


def last_kernel(mine_a, got_a, mine_b, got_b, out_ref):
    parity = lax.rem(lax.axis_index("grp"), 2)
    shape = out_ref.shape[:1] + out_ref.shape[2:]
    for at, mine, got in ((parity, mine_a, got_a), (1 - parity, mine_b, got_b)):
        total = mine[...] + got[...].astype(jnp.float32)
        out_ref[:, at] = total.astype(jnp.bfloat16).reshape(shape)


def router_kernel(local, capacity, score_ref, meta_ref, w_ref, out_ref):
    tokens = out_ref.shape[0]
    found = jnp.sum(score_ref[...], axis=1)
    scores = []
    for l in range(local):
        rank = meta_ref[l, 2].astype(jnp.int32)
        at = jnp.maximum(rank + (l * capacity - 1), 0)
        value = jnp.take_along_axis(found, at, axis=1, mode="promise_in_bounds")
        scores.append(jnp.where(rank > 0, value, 0.0))
    mean = sum(
        jnp.sum(meta_ref[l, 1] * scores[l], axis=0, keepdims=True) for l in range(local)
    ) * (1.0 / route_scale)
    grads = jnp.concatenate(
        [
            meta_ref[l, 1] * (1.0 - meta_ref[l, 0]) * (scores[l] - mean)
            for l in range(local)
        ],
        axis=0,
    ).astype(jnp.bfloat16)
    out_ref[...] = contract_rows(grads, w_ref[...])[:tokens].astype(jnp.bfloat16)


def cost(flops, nbytes):
    return pl.CostEstimate(flops=flops, bytes_accessed=nbytes, transcendentals=0)


def struct(shape, dtype):
    return jax.ShapeDtypeStruct(shape, dtype)


def held(x):
    return pltpu.with_memory_space_constraint(x, pltpu.VMEM)


def away_from_vmem(x):
    return pltpu.with_memory_space_constraint(x, pltpu.HBM)


def kept(shape, dtype):
    return pltpu.VMEM(shape, dtype)


def token_plan(out_grad, expert_ids, router_logits, router_weight, expert_weight, hidden_saved):
    group_rows, features = out_grad.shape
    groups, ep_count = lax.axis_size("grp"), lax.axis_size("ep")
    local, _, width = expert_weight.shape
    slot_count = hidden_saved.shape[1]
    capacity = slot_count // (local * groups)
    span = groups * capacity
    tokens = groups * group_rows
    bf16, f32 = jnp.bfloat16, jnp.float32
    vmem = pl.BlockSpec(memory_space=pltpu.VMEM)
    hbm = pl.BlockSpec(memory_space=pltpu.HBM)

    def limit(mib):
        return pltpu.CompilerParams(vmem_limit_bytes=mib * 2**20)

    packed, meta = pl.pallas_call(
        functools.partial(pack_kernel, local),
        out_shape=(
            pltpu.VMEM((group_rows, features + LANES), bf16),
            pltpu.VMEM((local, 3, groups, LANES), f32),
        ),
        in_specs=[hbm] * 3,
        out_specs=(vmem, vmem),
        scratch_shapes=[
            pltpu.VMEM(expert_ids.shape[::-1], jnp.int32),
            pltpu.VMEM(router_logits.shape[::-1], f32),
            pltpu.SemaphoreType.DMA((3,)),
        ],
        compiler_params=limit(2),
        name="pack",
    )(away_from_vmem(expert_ids.T), away_from_vmem(router_logits.T), away_from_vmem(out_grad))
    blocks = [held(b) for b in gather_blocks(packed)]

    saved_shape = (local, groups // 2, 2, capacity, width)
    sums = [kept((local, span // 4, width), bf16)] * 2
    work = slot_count * features * width
    saved_hbm = away_from_vmem(hidden_saved.reshape(saved_shape))
    half_weights, half_saved = pl.pallas_call(
        load_kernel,
        out_shape=(kept(expert_weight.shape, bf16), kept(saved_shape, bf16)),
        in_specs=[vmem, hbm, hbm],
        out_specs=(vmem, vmem),
        scratch_shapes=[pltpu.SemaphoreType.DMA((2,))],
        compiler_params=limit(2),
        cost_estimate=cost(work // 2, 8 * 2**20),
        name="load",
    )(blocks[0], away_from_vmem(expert_weight), saved_hbm)

    core_pairs = [(i, i ^ 1) for i in range(ep_count)]
    chip_pairs = [(i, i ^ 2) for i in range(ep_count)]

    def summed(kernel, keep, got):
        return pl.pallas_call(
            kernel,
            out_shape=(kept((span // 4, width), f32), kept((span // 4, width), bf16)),
            in_specs=[vmem] * 2,
            out_specs=(vmem,) * 2,
            compiler_params=limit(2),
        )(held(keep), held(got))

    weights, saved, projection, keep_a, send_a, score_a = pl.pallas_call(
        functools.partial(first_kernel, groups, capacity),
        out_shape=(
            kept(expert_weight.shape, bf16),
            kept(saved_shape, bf16),
            kept(router_weight.shape, bf16),
            kept((span // 2, width), bf16),
            kept((span // 2, width), bf16),
            kept((groups // 2, LANES), f32),
        ),
        in_specs=[vmem] * (groups // 2) + [hbm] * 3 + [vmem] * 2,
        out_specs=(vmem,) * 6,
        scratch_shapes=[pltpu.SemaphoreType.DMA((3,))],
        input_output_aliases={groups // 2 + 3: 0, groups // 2 + 4: 1},
        compiler_params=limit(8),
        cost_estimate=cost(work, 4 * 2**20),
        name="first",
    )(
        *blocks[0::2],
        away_from_vmem(expert_weight),
        saved_hbm,
        away_from_vmem(router_weight),
        held(half_weights),
        held(half_saved),
    )
    got_a = lax.ppermute(send_a, "ep", chip_pairs)

    keep_b, send_b, score = pl.pallas_call(
        functools.partial(second_kernel, local, groups, capacity),
        out_shape=(*sums, kept((groups // 2, 2, ep_count, LANES), f32)),
        in_specs=[vmem] * (groups // 2 + 3),
        out_specs=(vmem,) * 3,
        compiler_params=limit(8),
        cost_estimate=cost(work, 4 * 2**20),
        name="second",
    )(*blocks[1::2], held(weights), held(saved), held(score_a))
    got_b = lax.ppermute(send_b, "ep", core_pairs)
    from_all = lax.all_to_all(
        score.reshape(groups * ep_count, 1, LANES), ("grp", "ep"), 0, 0, tiled=True
    )
    mine_b, away_b = summed(pair_kernel, keep_b, got_b)
    last_b = lax.ppermute(away_b, "ep", chip_pairs)
    mine_a, away_a = summed(split_kernel, keep_a, got_a)
    last_a = lax.ppermute(away_a, "ep", core_pairs)

    parts = 4
    weight_grad, projection = pl.pallas_call(
        functools.partial(weight_kernel, local, groups, capacity, parts),
        out_shape=(struct((local, features, width), bf16), kept(router_weight.shape, bf16)),
        in_specs=[vmem] * (groups + 2),
        out_specs=(hbm, vmem),
        scratch_shapes=[
            pltpu.VMEM((features, tokens), bf16),
            pltpu.VMEM((features, span), bf16),
            pltpu.VMEM((local, features, width), bf16),
            pltpu.SemaphoreType.DMA((local * parts,)),
        ],
        compiler_params=limit(12),
        cost_estimate=cost(2 * slot_count * features * width, 6 * 2**20),
        name="weight",
    )(*blocks, held(saved.reshape(local, span, width)), held(projection))

    hidden_grad = pl.pallas_call(
        last_kernel,
        out_shape=struct((groups // 4, 2, capacity, width), bf16),
        in_specs=[vmem] * 4,
        out_specs=vmem,
        compiler_params=limit(2),
        name="last",
    )(held(mine_a), held(last_a), held(mine_b), held(last_b)).reshape(1, span // 2, width)

    input_grad = pl.pallas_call(
        functools.partial(router_kernel, local, capacity),
        out_shape=struct((group_rows, features), bf16),
        in_specs=[vmem] * 3,
        out_specs=vmem,
        compiler_params=limit(2),
        name="router",
    )(held(from_all.reshape(groups, ep_count, LANES)), held(meta), held(projection))
    return (weight_grad, hidden_grad, input_grad)


def body(out_grad, expert_ids, router_logits, router_weight, expert_weight, hidden_saved):
    groups, ep_count = lax.axis_size("grp"), lax.axis_size("ep")
    rows, experts = router_logits.shape
    slots = hidden_saved.shape[1]
    local = expert_weight.shape[0]
    fits = (
        rows * groups <= slots
        and groups % 8 == 0
        and groups & (groups - 1) == 0
        and (local, ep_count) == (2, 4)
        and rows % 16 == 0
        and slots // groups <= LANES
        and 2 * experts <= LANES
    )
    plan = token_plan if fits else slot_plan
    return plan(
        out_grad, expert_ids, router_logits, router_weight, expert_weight, hidden_saved
    )


def solution(mesh):
    in_specs = (
        P("grp", "ep"),
        P("grp", None),
        P("grp", None),
        P(None, "ep"),
        P("grp", "ep", None),
        P("grp", None, None),
    )
    out_specs = (P("grp", "ep", None), P("grp", "ep", None), P("grp", "ep"))
    return jax.shard_map(body, mesh=mesh, in_specs=in_specs, out_specs=out_specs, check_vma=False)
```
